32 devices in a mesh: ens: 16 (over z, y, core), batch: 2 (over x).
Axes of the slice: x: 2, y: 2, z: 4, core: 2. Of those that a mesh axis runs over, the one named last changes fastest.
Arguments:
- replay_obs: bfloat16 [512, 1024], P('batch'), may hold values from -4.1875 to 4.1875
- replay_next: bfloat16 [512, 1024], P('batch'), may hold values from -4.1875 to 4.1875
- batch_rows: int32 [64], P('batch'), may hold values from 0 to 255
- data_action: int32 [64], P('batch'), may hold values from 0 to 255
- next_action: int32 [64], P('batch'), may hold values from 0 to 255
- sampled_actions: int32 [64, 16], P('batch'), may hold values from 0 to 255
- reward: float32 [64], P('batch'), may hold values from -6 to 6
- next_logp: float32 [64], P('batch'), may hold values from -6 to 2
- action_table: bfloat16 [256, 1024], replicated, may hold values from -4.1875 to 4.1875
- w1: bfloat16 [16, 4096, 1024], P('ens'), may hold values from -0.1875 to 0.1875
- w2: float32 [16, 4096], P('ens'), may hold values from -0.375 to 0.375
Outputs:
- grad_w1: float32 [16, 4096, 1024], P('ens', 'batch')
- grad_w2: float32 [16, 4096], P('ens')
- critic_stats: float32 [16, 3], P('ens')
The draws below stay inside these ranges and needn't reach their ends.
Inputs may be any that keep to these rules, and one draw needn't show every extreme that they name: `batch_rows`: each entry is a row of the own block of 256 replay rows that holds its state.
All inputs are finite; a program needn't handle non-finite values.
Results may differ from the reference program's by a relative error of at most 0.0045.
Values may be sent and summed in bfloat16 or wider, within the bound.
A program may use at most 128 MiB of HBM per device.

```python
import jax
import jax.numpy as jnp
from jax import lax

D = 1024
H = 4096
NACT = 256
A = 16
S_DEV = 32
BUF_DEV = 256
ENS = 16
STATES = 64
N_BATCH = 2


def touch_ends(array, key, least, high):
    index_at = [jax.random.randint(jax.random.fold_in(key, axis), (), 0, length) for axis, length in enumerate(array.shape)]
    longest = array.shape.index(max(array.shape))
    next_to = index_at[:longest] + [(index_at[longest] + 1) % array.shape[longest]] + index_at[longest + 1:]
    return array.at[tuple(index_at)].set(least).at[tuple(next_to)].set(high)


def shard_levels(own_key, shape, shards, least, top_value):
    factor_of, own = 1.0, jax.random.fold_in(own_key, 6)
    for axis_at, shards_of in shards:
        steps = jnp.exp(jax.random.uniform(jax.random.fold_in(own, axis_at), (shards_of,), jnp.float32, least / len(shards), top_value / len(shards)))
        factor_of = factor_of * jnp.repeat(steps, shape[axis_at] // shards_of).reshape([-1 if axis == axis_at else 1 for axis in range(len(shape))])
    return factor_of


def scatter_about(stream_key, extent, deviation, bound, pieces=(), kind=jnp.bfloat16):
    array = jax.random.normal(stream_key, extent, jnp.float32) * deviation
    if len(pieces) > 0:
        array = shard_levels(stream_key, extent, pieces, -0.22, 0.18) * array
    return jnp.clip(array, min=-bound, max=bound).astype(kind)


def setup_inputs(seed: int = 0) -> dict:
    key_list = jax.random.split(jax.random.key(seed), 12)
    return {
        "replay_obs": scatter_about(key_list[0], (N_BATCH * BUF_DEV, D), 0.7, 4.1875, ((0, 2),)),
        "replay_next": scatter_about(key_list[1], (N_BATCH * BUF_DEV, D), 0.7, 4.1875, ((0, 2),)),
        "batch_rows": touch_ends(jax.random.randint(key_list[2], (STATES,), 0, BUF_DEV), jax.random.fold_in(key_list[2], 1), 0, BUF_DEV - 1).astype(jnp.int32),
        "data_action": touch_ends(jax.random.randint(key_list[3], (STATES,), 0, NACT), jax.random.fold_in(key_list[3], 1), 0, NACT - 1).astype(jnp.int32),
        "next_action": touch_ends(jax.random.randint(key_list[4], (STATES,), 0, NACT), jax.random.fold_in(key_list[4], 1), 0, NACT - 1).astype(jnp.int32),
        "sampled_actions": touch_ends(jax.random.randint(key_list[5], (STATES, A), 0, NACT), jax.random.fold_in(key_list[5], 1), 0, NACT - 1).astype(jnp.int32),
        "reward": scatter_about(key_list[6], (STATES,), 1.0, 6.0, ((0, 2),), jnp.float32),
        "next_logp": jnp.clip(-6.0 + 8.0 * jax.random.uniform(key_list[7], (STATES,), jnp.float32) ** shard_levels(key_list[7], (STATES,), ((0, 2),), -0.2, 0.2), -6.0, 2.0),
        "action_table": scatter_about(key_list[8], (NACT, D), 0.7, 4.1875),
        "w1": scatter_about(key_list[9], (ENS, H, D), D ** -0.5, 0.1875, ((0, 16),)),
        "w2": scatter_about(key_list[10], (ENS, H), (4.0 / H ** 0.5), 0.375, ((0, 16),), jnp.float32),
    }


discount = 0.99
entropy_temp = 0.2
penalty_weight = 1.0
diversity_weight = 1000.0

def silu_terms(preact):
    sigmoid_v = jax.nn.sigmoid(preact)
    silu_out = preact * sigmoid_v
    slope_one = sigmoid_v * (1.0 + preact * (1.0 - sigmoid_v))
    return (silu_out, slope_one, sigmoid_v)

def reference(replay_obs, replay_next, batch_rows, data_action, next_action, sampled_actions, reward, next_logp, action_table, w1, w2):
    owners = jnp.arange(STATES, dtype=jnp.int32) // S_DEV
    row_ids = owners * BUF_DEV + batch_rows.astype(jnp.int32)
    obs_rows = jnp.take(replay_obs, row_ids, axis=0).astype(jnp.float32)
    next_rows = jnp.take(replay_next, row_ids, axis=0).astype(jnp.float32)
    table_f = action_table.astype(jnp.float32)
    x_next = (next_rows + jnp.take(table_f, next_action, axis=0)).astype(jnp.bfloat16)
    x_data = (obs_rows + jnp.take(table_f, data_action, axis=0)).astype(jnp.bfloat16)
    x_samp = (obs_rows[:, None, :] + jnp.take(table_f, sampled_actions, axis=0)).astype(jnp.bfloat16)
    x_samp = x_samp.reshape(STATES * A, D)

    def data_pass(weight, readout):
        preact = jnp.dot(x_data, weight.T, preferred_element_type=jnp.float32)
        silu_out, slope_one, sigmoid_v = silu_terms(preact)
        coeffs = (readout * slope_one).astype(jnp.bfloat16)
        grad_in = jnp.dot(coeffs, weight, preferred_element_type=jnp.float32)
        in_norm = jnp.sqrt(lax.optimization_barrier(jnp.sum(grad_in * grad_in, axis=-1, keepdims=True)) + 1.0)
        return (preact, silu_out, slope_one, sigmoid_v, coeffs, in_norm, grad_in / in_norm)

    def forward(params):
        weight, readout = params
        pre_next = jnp.dot(x_next, weight.T, preferred_element_type=jnp.float32)
        q_next = lax.optimization_barrier(jnp.sum(silu_terms(pre_next)[0] * readout, axis=-1))
        unit_dir = data_pass(weight, readout)[6]
        return (q_next, unit_dir)
    q_next_all, units = lax.map(forward, (w1, w2))
    target_floor = lax.optimization_barrier(jnp.min(q_next_all, axis=0))
    target = reward + discount * (target_floor - entropy_temp * next_logp)
    spread = lax.optimization_barrier(jnp.sum(units, axis=0))

    def backward(params):
        weight, readout = params
        preact, silu_out, slope_one, sigmoid_v, coeffs, in_norm, unit_dir = data_pass(weight, readout)
        q_data = lax.optimization_barrier(jnp.sum(silu_out * readout, axis=-1))
        pre_samp = jnp.dot(x_samp, weight.T, preferred_element_type=jnp.float32)
        silu_samp, slope_samp, _ = silu_terms(pre_samp)
        q_samp = lax.optimization_barrier(jnp.sum(silu_samp * readout, axis=-1)).reshape(STATES, A)
        td_gap = q_data - target
        log_mass = jnp.log(lax.optimization_barrier(jnp.sum(jnp.exp(q_samp), axis=-1)))
        action_prob = jnp.exp(q_samp - log_mass[:, None])
        div_row = lax.optimization_barrier(jnp.sum(unit_dir * (spread - unit_dir), axis=-1))
        stats = jnp.stack([jnp.sum(td_gap * td_gap), jnp.sum(log_mass - q_data), jnp.sum(div_row)]) / STATES
        dq_data = (2.0 * td_gap - penalty_weight) / STATES
        dq_samp = (penalty_weight * action_prob / STATES).reshape(STATES * A)
        dunit = 2.0 * diversity_weight / (ENS - 1) / STATES * (spread - unit_dir)
        dgrad = ((dunit - unit_dir * lax.optimization_barrier(jnp.sum(unit_dir * dunit, axis=-1, keepdims=True))) / in_norm).astype(jnp.bfloat16)
        dcoef = jnp.dot(dgrad, weight.T, preferred_element_type=jnp.float32)
        curve_two = sigmoid_v * (1.0 - sigmoid_v) * (2.0 + preact * (1.0 - 2.0 * sigmoid_v))
        dpre_data = (dq_data[:, None] * readout * slope_one + dcoef * readout * curve_two).astype(jnp.bfloat16)
        dpre_samp = (dq_samp[:, None] * readout * slope_samp).astype(jnp.bfloat16)
        grad_v = lax.optimization_barrier(jnp.sum(dq_data[:, None] * silu_out, axis=0)) + lax.optimization_barrier(jnp.sum(dq_samp[:, None] * silu_samp, axis=0)) + lax.optimization_barrier(jnp.sum(dcoef * slope_one, axis=0))
        grad_w = jnp.dot(dpre_data.T, x_data, preferred_element_type=jnp.float32)
        grad_w = grad_w + jnp.dot(dpre_samp.T, x_samp, preferred_element_type=jnp.float32)
        grad_w = grad_w + jnp.dot(coeffs.T, dgrad, preferred_element_type=jnp.float32)
        return (grad_w, grad_v, stats)
    grad_w1, grad_w2, critic_stats = lax.map(backward, (w1, w2))
    return (grad_w1, grad_w2, critic_stats)
```

```python
import functools

import jax
import jax.numpy as jnp
from jax import lax
from jax.experimental import pallas as pl
from jax.experimental.pallas import tpu as pltpu
from jax.sharding import PartitionSpec as P

discount = 0.99
entropy_temp = 0.2
penalty_weight = 1.0
diversity_weight = 1000.0

MESH = pl.DeviceIdType.MESH
F32 = jnp.float32
BF16 = jnp.bfloat16
CHUNK = 256
LANES = 128
VMEM_LIMIT = 60 * 1024 * 1024
VMEM_LIMIT_2 = 60 * 1024 * 1024


def dot_t(a, b):
    return lax.dot_general(a, b, (((1,), (1,)), ((), ())), preferred_element_type=F32)


def sigmoid(x):
    return 0.5 * jnp.tanh(0.5 * x) + 0.5


def kernel(
    n_ens, per_dev, samples, critics_total,
    rows_ref, next_act_ref, data_act_ref, samp_act_ref, reward_ref, logp_ref, w2_ref,
    obs_hbm, next_hbm, table_hbm, w1_ref,
    lhs_hbm, rhs_hbm, gv_ref, stat_ref,
    obs_ref, next_ref, table_ref, acts_ref, aux_ref, wbuf, xcat, xnext, acts_in, aux_in, sel, sel_dq, ptab,
    pbuf_a, pbuf_b, base, pcat, vb, cot, sbuf, ubuf,
    gpart, gsend, grecv, qpart, qrecv, unit, usend, urecv, qmine, qall, spread_mine, spread_all,
    dgrad, div_out, div_in, dcoef_buf, gvsamp, gvbuf, lhs, tabd,
    in_sem, w_sem, a_send, a_recv, g_send, g_recv, u_send, u_recv, m_send, m_recv, s_send, s_recv,
    d_send, d_recv, v_send, v_recv, o_sem,
):
    e = lax.axis_index("ens")
    b = lax.axis_index("batch")
    peer = 1 - b
    states = 2 * per_dev
    block = 2 * states
    nact = table_ref.shape[0]
    width = table_ref.shape[1]
    cols = acts_ref.shape[1]
    samp_cols = cols - block
    groups = samp_cols // LANES
    half = wbuf.shape[0]
    chunks = half // CHUNK
    pair = {"ens": e, "batch": peer}

    def other(k):
        return {"ens": lax.rem(e + k, n_ens), "batch": b}

    barrier = pltpu.get_barrier_semaphore()
    pl.semaphore_signal(barrier, inc=1, device_id=pair, device_id_type=MESH)

    def greet(k, carry):
        pl.semaphore_signal(barrier, inc=1, device_id=other(k), device_id_type=MESH)
        return carry

    lax.fori_loop(1, n_ens, greet, 0)

    loads = [
        pltpu.make_async_copy(obs_hbm, obs_ref, in_sem.at[0]),
        pltpu.make_async_copy(table_hbm, table_ref, in_sem.at[1]),
        pltpu.make_async_copy(next_hbm, next_ref, in_sem.at[2]),
    ]
    for copy in loads:
        copy.start()

    def w_copy(c):
        return pltpu.make_async_copy(
            w1_ref.at[0, pl.ds(b * half + c * CHUNK, CHUNK), :],
            wbuf.at[pl.ds(c * CHUNK, CHUNK), :],
            w_sem.at[c],
        )

    for c in range(chunks):
        w_copy(c).start()

    own_rows = pl.ds(pl.multiple_of(b * per_dev, per_dev), per_dev)
    peer_rows = pl.ds(pl.multiple_of(peer * per_dev, per_dev), per_dev)

    def one_hot(index_row, length):
        row = jnp.concatenate([index_row, jnp.zeros((1, LANES - per_dev), jnp.int32)], axis=1)
        hit = row == lax.broadcasted_iota(jnp.int32, (length, LANES), 0)
        return jnp.transpose(jnp.where(hit, 1.0, 0.0))[:per_dev, :].astype(BF16)

    pick = one_hot(rows_ref[...], obs_ref.shape[0])
    act_rows = [next_act_ref[...], data_act_ref[...]]
    act_rows += [samp_act_ref[i:i + 1, :] for i in range(samples)]

    def place(part):
        return [jnp.where(b == 0, part, jnp.zeros_like(part)), jnp.where(b == 0, jnp.zeros_like(part), part)]

    for j in range(cols // block):
        acts_ref[:, j * block:(j + 1) * block] = jnp.concatenate(
            place(act_rows[2 * j]) + place(act_rows[2 * j + 1]), axis=1
        )
    blank = jnp.zeros((1, states), F32)
    aux_ref[0:1, :] = jnp.concatenate([blank] + place(reward_ref[...]), axis=1)
    aux_ref[1:2, :] = jnp.concatenate([blank] + place(logp_ref[...]), axis=1)
    loads[0].wait()
    xcat[own_rows, :] = jnp.dot(pick, obs_ref[...], preferred_element_type=F32).astype(BF16)
    loads[1].wait()
    loads[2].wait()
    moved = jnp.dot(one_hot(next_act_ref[...], nact), table_ref[...], preferred_element_type=F32)
    moved = moved + jnp.dot(pick, next_ref[...], preferred_element_type=F32)
    xnext[own_rows, :] = moved.astype(BF16)
    pl.semaphore_wait(barrier, n_ens)

    def remote(src, dst, send, recv, to):
        return pltpu.make_async_remote_copy(
            src_ref=src, dst_ref=dst, send_sem=send, recv_sem=recv,
            device_id=to, device_id_type=MESH,
        )

    first = [
        remote(acts_ref, acts_in, a_send.at[0], a_recv.at[0], pair),
        remote(xcat.at[own_rows, :], xcat.at[own_rows, :], a_send.at[1], a_recv.at[1], pair),
        remote(xnext.at[own_rows, :], xnext.at[own_rows, :], a_send.at[2], a_recv.at[2], pair),
        remote(aux_ref, aux_in, a_send.at[3], a_recv.at[3], pair),
    ]
    for copy in first:
        copy.start()

    def table_step(c, carry):
        rows = pl.ds(pl.multiple_of(c * CHUNK, CHUNK), CHUNK)
        w_copy(c).wait()
        ptab[rows, :] = (0.5 * dot_t(wbuf[rows, :], table_ref[...])).astype(BF16)
        v_row = w2_ref[0:1, pl.ds(pl.multiple_of(b * half + c * CHUNK, CHUNK), CHUNK)]
        vb[rows, :] = jnp.transpose(jnp.broadcast_to(v_row, (LANES, CHUNK)))
        return carry

    lax.fori_loop(0, chunks, table_step, 0)

    first[0].wait()
    acts = acts_ref[...] + acts_in[...]
    hit = acts[:, :block] == lax.broadcasted_iota(jnp.int32, (nact, block), 0)
    picked = jnp.transpose(jnp.where(hit, 1.0, 0.0))[states:, :].astype(BF16)
    tabd[...] = jnp.dot(picked, table_ref[...], preferred_element_type=F32)
    state_row = nact + lax.rem(lax.broadcasted_iota(jnp.int32, (1, LANES), 1), states)
    for j in range(groups):
        row = lax.broadcasted_iota(jnp.int32, (nact + block, LANES), 0)
        hit = jnp.logical_or(row == acts[:, block + j * LANES:block + (j + 1) * LANES], row == state_row)
        sel[:, j * LANES:(j + 1) * LANES] = jnp.where(hit, 1.0, 0.0).astype(BF16)

    lane = lax.broadcasted_iota(jnp.int32, (1, block), 1)
    low = lane < states
    first[1].wait()
    xcat[states:, :] = (xcat[:states, :].astype(F32) + tabd[...]).astype(BF16)

    def chunk_rows(c):
        return slice(c * CHUNK, (c + 1) * CHUNK)

    def data_matmul(c):
        pcat[chunk_rows(c), :] = dot_t(wbuf[chunk_rows(c), :], xcat[...])

    def data_forward(c, q_acc):
        rows = chunk_rows(c)
        pre = pcat[rows, :]
        base[rows, :] = 0.5 * jnp.where(low, pre, pltpu.roll(pre, states, 1))
        v = vb[rows, :]
        sig = sigmoid(pre)
        silu = pre * sig
        weighted = v * (sig * (1.0 + (pre - silu)))
        lhs[rows, nact + block:] = jnp.where(low, 0.0, weighted).astype(BF16)
        cot[:, rows] = jnp.transpose(weighted)[states:, :].astype(BF16)
        return q_acc + jnp.sum(silu * v, axis=0, keepdims=True)

    q_data = jnp.zeros((1, block), F32)
    data_matmul(0)
    for c in range(chunks):
        if c + 1 < chunks:
            data_matmul(c + 1)
        q_data = data_forward(c, q_data)
    gpart[...] = jnp.dot(cot[...], wbuf[...], preferred_element_type=F32)
    gsend[...] = gpart[peer_rows, :].astype(gsend.dtype)
    qpart[:, :block] = q_data
    second = [
        remote(qpart.at[:, :block], qrecv.at[:, :block], g_send.at[0], g_recv.at[0], pair),
        remote(gsend, grecv, g_send.at[1], g_recv.at[1], pair),
        remote(qpart.at[:, block:], qrecv.at[:, block:], g_send.at[2], g_recv.at[2], pair),
    ]
    second[1].start()

    first[2].wait()

    def next_forward(c, acc):
        rows = pl.ds(pl.multiple_of(c * 2 * CHUNK, 2 * CHUNK), 2 * CHUNK)
        pre = dot_t(wbuf[rows, :], xnext[...])
        silu = pre * sigmoid(pre)
        return acc + jnp.sum(silu * vb[rows, :states], axis=0, keepdims=True)

    q_next = lax.fori_loop(0, chunks // 2, next_forward, jnp.zeros((1, states), F32))
    qpart[:, :states] = q_next
    second[0].start()

    def samp_matmul(c, buf):
        rows = pl.ds(pl.multiple_of(c * CHUNK, CHUNK), CHUNK)
        buf[...] = jnp.dot(ptab[rows, :], sel[:nact, :], preferred_element_type=F32)

    SUB = 32

    def samp_forward(c, buf, q_acc):
        q_acc = list(q_acc)
        for r in range(CHUNK // SUB):
            here = slice(r * SUB, (r + 1) * SUB)
            there = pl.ds(pl.multiple_of(c * CHUNK + r * SUB, SUB), SUB)
            v = vb[there, :]
            start = base[there, :]
            for j in range(groups):
                at = slice(j * LANES, (j + 1) * LANES)
                h = buf[here, at] + start
                t = jnp.tanh(h)
                m = h * t
                silu = h + m
                slope = (1.0 + t) * (1.0 + (h - m))
                sbuf[there, at] = slope.astype(BF16)
                ubuf[there, at] = silu.astype(BF16)
                sv = silu * v
                part = sv[0:8]
                for i in range(1, SUB // 8):
                    part = part + sv[8 * i:8 * i + 8]
                q_acc[j] = q_acc[j] + part
        return tuple(q_acc)

    def samp_pair(k, q_acc):
        samp_matmul(2 * k + 1, pbuf_b)
        q_acc = samp_forward(2 * k, pbuf_a, q_acc)
        samp_matmul(lax.rem(2 * k + 2, chunks), pbuf_a)
        return samp_forward(2 * k + 1, pbuf_b, q_acc)

    q_acc = (jnp.zeros((8, LANES), F32),) * groups
    cut_one, cut_two = chunks // 8, (chunks // 8) * 3
    samp_matmul(0, pbuf_a)
    q_acc = lax.fori_loop(0, cut_one, samp_pair, q_acc)

    def q_copy(k):
        return remote(qmine, qall.at[k], m_send.at[k], m_recv.at[k], other(k))

    def u_copy(k):
        return remote(
            usend.at[lax.rem(e + k, n_ens)], urecv.at[k], u_send.at[k], u_recv.at[k], other(k)
        )

    def s_copy(k):
        return remote(spread_mine, spread_all.at[e], s_send.at[k], s_recv.at[k], other(k))

    def start_all(make):
        def go(k, carry):
            make(k).start()
            return carry
        lax.fori_loop(1, n_ens, go, 0)

    def wait_all(make):
        def go(k, carry):
            make(k).wait()
            return carry
        lax.fori_loop(1, n_ens, go, 0)

    second[1].wait()
    grad_in = gpart[own_rows, :] + grecv[...].astype(F32)
    norm_sq = jnp.sum(grad_in * grad_in, axis=-1, keepdims=True) + 1.0
    in_norm = jnp.sqrt(norm_sq)
    unit[...] = grad_in / in_norm
    piece = usend.shape[1]
    per_col = per_dev // piece
    for p in range(n_ens):
        c0, r0 = p // per_col, (p % per_col) * piece
        usend[p] = unit[r0:r0 + piece, c0 * LANES:(c0 + 1) * LANES].astype(BF16)
    start_all(u_copy)
    second[0].wait()
    q0 = qpart[:, :block] + qrecv[:, :block]
    qmine[...] = jnp.broadcast_to(q0, qmine.shape)
    start_all(q_copy)

    q_acc = lax.fori_loop(cut_one, cut_two, samp_pair, q_acc)

    wait_all(u_copy)
    total = usend[e].astype(F32)
    for k in range(1, n_ens):
        total = total + urecv[k].astype(F32)
    spread_mine[...] = total.astype(BF16)
    spread_all[e] = total.astype(BF16)
    start_all(s_copy)
    q_acc = lax.fori_loop(cut_two, chunks // 2, samp_pair, q_acc)
    for j in range(groups):
        qpart[:, block + j * LANES:block + (j + 1) * LANES] = jnp.sum(q_acc[j], axis=0, keepdims=True)
    second[2].start()
    wait_all(q_copy)
    floor = qmine[...]
    for k in range(1, n_ens):
        floor = jnp.minimum(floor, qall[k])
    floor = pltpu.roll(floor, states, 1)[0:1, :]
    first[3].wait()
    aux = aux_ref[...] + aux_in[...]
    target = aux[0:1, :] + discount * (floor - entropy_temp * aux[1:2, :])
    td_gap = q0 - target
    dq_data = jnp.where(low, 0.0, (2.0 * td_gap - penalty_weight) / states)

    wait_all(s_copy)
    scale = 2.0 * diversity_weight / (critics_total - 1) / states
    for p in range(n_ens):
        c0, r0 = p // per_col, (p % per_col) * piece
        gpart[r0:r0 + piece, c0 * LANES:(c0 + 1) * LANES] = spread_all[p].astype(F32)
    unit_dir = unit[...]
    away = gpart[:per_dev, :] - unit_dir
    div_row = jnp.sum(unit_dir * away, axis=-1, keepdims=True)
    dg = scale * (away - unit_dir * div_row) / in_norm
    dg_rows = pl.ds(pl.multiple_of(states + b * per_dev, per_dev), per_dev)
    dgrad[:states, :] = jnp.zeros((states, width), BF16)
    dgrad[dg_rows, :] = dg.astype(BF16)
    div_sum = jnp.sum(div_row, axis=0, keepdims=True)
    div_out[...] = jnp.broadcast_to(div_sum, div_out.shape)
    third = [
        remote(dgrad.at[dg_rows, :], dgrad.at[dg_rows, :], d_send.at[0], d_recv.at[0], pair),
        remote(div_out, div_in, d_send.at[1], d_recv.at[1], pair),
    ]
    for copy in third:
        copy.start()
    second[2].wait()
    q_samp = qpart[:, block:] + qrecv[:, block:]
    exps = jnp.exp(q_samp)
    mass = exps[:, :block]
    for j in range(1, groups):
        mass = mass + exps[:, j * block:(j + 1) * block]
    mass = mass + pltpu.roll(mass, states, 1)
    log_mass = jnp.log(mass)
    tiled = jnp.concatenate([log_mass] * groups, axis=1)
    dq_samp = penalty_weight * jnp.exp(q_samp - tiled) / states
    for j in range(groups):
        at = slice(j * LANES, (j + 1) * LANES)
        sel_dq[:, at] = (sel[:, at].astype(F32) * (0.5 * dq_samp[:, at])).astype(BF16)

    def samp_gv(c, carry):
        there = pl.ds(pl.multiple_of(c * SUB * 2, SUB * 2), SUB * 2)
        total = ubuf[there, :LANES].astype(F32) * dq_samp[:, :LANES]
        for j in range(1, groups):
            at = slice(j * LANES, (j + 1) * LANES)
            total = total + ubuf[there, at].astype(F32) * dq_samp[:, at]
        gvsamp[there, :] = total
        return carry

    def samp_step(c, carry):
        rows = pl.ds(pl.multiple_of(c * 2 * CHUNK, 2 * CHUNK), 2 * CHUNK)
        grads = dot_t(sbuf[rows, :], sel_dq[...])
        v = vb[rows, :]
        for j in range((nact + block) // LANES):
            at = slice(j * LANES, (j + 1) * LANES)
            lhs[rows, at] = (v * grads[:, at]).astype(BF16)
        return carry

    lax.fori_loop(0, half // (SUB * 2), samp_gv, 0)
    steps = chunks // 2
    lax.fori_loop(0, steps // 2, samp_step, 0)
    for copy in third:
        copy.wait()
    rhs_out = [
        pltpu.make_async_copy(table_ref, rhs_hbm.at[:nact], in_sem.at[0]),
        pltpu.make_async_copy(xcat, rhs_hbm.at[nact:nact + block], in_sem.at[1]),
        pltpu.make_async_copy(dgrad, rhs_hbm.at[nact + block:], in_sem.at[2]),
    ]
    for copy in rhs_out:
        copy.start()

    def dcoef_matmul(c):
        dcoef_buf[chunk_rows(c), :] = dot_t(wbuf[chunk_rows(c), :], dgrad[...])

    def data_backward(c):
        rows = chunk_rows(c)
        dcoef = dcoef_buf[rows, :]
        pre = pcat[rows, :]
        v = vb[rows, :]
        sig = sigmoid(pre)
        silu = pre * sig
        slope = sig * (1.0 + (pre - silu))
        curve = sig * (1.0 - sig) * (2.0 + pre * (1.0 - 2.0 * sig))
        dcoef_buf[rows, :] = v * (dq_data * slope + dcoef * curve)
        gv = gvsamp[rows, :] + jnp.where(low, 0.0, dq_data * silu + dcoef * slope)
        gvbuf[b, c:c + 1, :] = jnp.sum(jnp.transpose(gv), axis=0, keepdims=True)

    dcoef_matmul(0)
    for c in range(chunks):
        if c + 1 < chunks:
            dcoef_matmul(c + 1)
        data_backward(c)
    last = remote(gvbuf.at[b], gvbuf.at[b], v_send, v_recv, pair)
    last.start()
    lax.fori_loop(steps // 2, steps, samp_step, 0)

    def lhs_copy(c):
        rows = pl.ds(c * CHUNK, CHUNK)
        return pltpu.make_async_copy(lhs.at[rows, :], lhs_hbm.at[rows, :], o_sem.at[c])

    mid = slice(nact, nact + block)
    for c in range(chunks):
        rows = chunk_rows(c)
        lhs[rows, mid] = jnp.where(low, lhs[rows, mid].astype(F32), dcoef_buf[rows, :]).astype(BF16)
        lhs_copy(c).start()

    td_total = jnp.sum(jnp.where(low, 0.0, td_gap * td_gap), axis=1, keepdims=True)
    gap_total = jnp.sum(jnp.where(low, 0.0, log_mass - q0), axis=1, keepdims=True)
    div_total = div_out[0:1, :] + div_in[0:1, :]
    stats = jnp.where(lane == 0, td_total, jnp.where(lane == 1, gap_total, div_total))
    stat_ref[...] = (stats / states)[:, :3]
    last.wait()
    for i in range(2):
        for c in range(chunks):
            at = i * half + c * CHUNK
            gv_ref[:, at:at + CHUNK] = gvbuf[i, c:c + 1, :]
    for copy in rhs_out:
        copy.wait()
    for c in range(chunks):
        lhs_copy(c).wait()


def finish(lhs_ref, rhs_ref, gv_ref, stat_ref, out_ref, gv_out, stat_out):
    out_ref[0] = jnp.dot(lhs_ref[...], rhs_ref[...], preferred_element_type=F32)

    @pl.when(pl.program_id(0) == 0)
    def small():
        gv_out[...] = gv_ref[...]
        stat_out[...] = stat_ref[...]


def body(
    replay_obs, replay_next, batch_rows, data_action, next_action, sampled_actions,
    reward, next_logp, action_table, w1, w2,
):
    per_dev = batch_rows.shape[0]
    samples = sampled_actions.shape[1]
    width = replay_obs.shape[1]
    hidden = w1.shape[1]
    n_batch = lax.axis_size("batch")
    n_ens = lax.axis_size("ens")
    if n_batch != 2 or w1.shape[0] != 1:
        raise ValueError("unsupported mesh")
    states = per_dev * n_batch
    block = 2 * states
    half = hidden // n_batch
    nact = action_table.shape[0]
    cols = (samples + 2) * states
    samp_cols = cols - block
    inner = nact + 2 * block
    chunks = half // CHUNK
    piece = per_dev * width // LANES // n_ens
    vmem = pl.BlockSpec(memory_space=pltpu.VMEM)
    anywhere = pl.BlockSpec(memory_space=pl.ANY)
    dma = pltpu.SemaphoreType.DMA
    lhs, rhs, gv, stats = pl.pallas_call(
        functools.partial(kernel, n_ens, per_dev, samples, n_ens * w1.shape[0]),
        out_shape=(
            jax.ShapeDtypeStruct((half, inner), BF16),
            jax.ShapeDtypeStruct((inner, width), BF16),
            jax.ShapeDtypeStruct((1, hidden), F32),
            jax.ShapeDtypeStruct((1, 3), F32),
        ),
        in_specs=[vmem] * 7 + [anywhere] * 4,
        out_specs=(anywhere, anywhere, vmem, vmem),
        scratch_shapes=[
            pltpu.VMEM(replay_obs.shape, BF16),
            pltpu.VMEM(replay_next.shape, BF16),
            pltpu.VMEM(action_table.shape, BF16),
            pltpu.VMEM((1, cols), jnp.int32),
            pltpu.VMEM((2, block), F32),
            pltpu.VMEM((half, width), BF16),
            pltpu.VMEM((block, width), BF16),
            pltpu.VMEM((states, width), BF16),
            pltpu.VMEM((1, cols), jnp.int32),
            pltpu.VMEM((2, block), F32),
            pltpu.VMEM((nact + block, samp_cols), BF16),
            pltpu.VMEM((nact + block, samp_cols), BF16),
            pltpu.VMEM((half, nact), BF16),
            pltpu.VMEM((CHUNK, samp_cols), F32),
            pltpu.VMEM((CHUNK, samp_cols), F32),
            pltpu.VMEM((half, block), F32),
            pltpu.VMEM((half, block), F32),
            pltpu.VMEM((half, LANES), F32),
            pltpu.VMEM((states, half), BF16),
            pltpu.VMEM((half, samp_cols), BF16),
            pltpu.VMEM((half, samp_cols), BF16),
            pltpu.VMEM((states, width), F32),
            pltpu.VMEM((per_dev, width), BF16),
            pltpu.VMEM((per_dev, width), BF16),
            pltpu.VMEM((1, cols), F32),
            pltpu.VMEM((1, cols), F32),
            pltpu.VMEM((per_dev, width), F32),
            pltpu.VMEM((n_ens, piece, LANES), BF16),
            pltpu.VMEM((n_ens, piece, LANES), BF16),
            pltpu.VMEM((8, block), F32),
            pltpu.VMEM((n_ens, 8, block), F32),
            pltpu.VMEM((piece, LANES), BF16),
            pltpu.VMEM((n_ens, piece, LANES), BF16),
            pltpu.VMEM((block, width), BF16),
            pltpu.VMEM((8, block), F32),
            pltpu.VMEM((8, block), F32),
            pltpu.VMEM((half, block), F32),
            pltpu.VMEM((half, LANES), F32),
            pltpu.VMEM((2, chunks, CHUNK), F32),
            pltpu.VMEM((half, inner), BF16),
            pltpu.VMEM((states, width), F32),
            dma((3,)), dma((chunks,)),
            dma((4,)), dma((4,)), dma((3,)), dma((3,)),
            dma((n_ens,)), dma((n_ens,)), dma((n_ens,)), dma((n_ens,)), dma((n_ens,)), dma((n_ens,)),
            dma((2,)), dma((2,)), dma, dma, dma((chunks,)),
        ],
        compiler_params=pltpu.CompilerParams(
            collective_id=0, has_side_effects=True, vmem_limit_bytes=VMEM_LIMIT
        ),
    )(
        batch_rows[None], next_action[None], data_action[None],
        sampled_actions.T, reward[None], next_logp[None], w2,
        replay_obs, replay_next, action_table, w1,
    )
    tile = half // 4
    small = pl.BlockSpec((1, hidden), lambda i: (0, 0))
    tiny = pl.BlockSpec((1, 3), lambda i: (0, 0))
    return pl.pallas_call(
        finish,
        grid=(half // tile,),
        out_shape=(
            jax.ShapeDtypeStruct((1, half, width), F32),
            jax.ShapeDtypeStruct((1, hidden), F32),
            jax.ShapeDtypeStruct((1, 3), F32),
        ),
        in_specs=[
            pl.BlockSpec((tile, inner), lambda i: (i, 0)),
            pl.BlockSpec((inner, width), lambda i: (0, 0)),
            small, tiny,
        ],
        out_specs=(pl.BlockSpec((1, tile, width), lambda i: (0, i, 0)), small, tiny),
        compiler_params=pltpu.CompilerParams(vmem_limit_bytes=VMEM_LIMIT_2),
    )(lhs, rhs, gv, stats)


def solution(mesh):
    return jax.shard_map(
        body,
        mesh=mesh,
        in_specs=(
            P("batch", None),
            P("batch", None),
            P("batch"),
            P("batch"),
            P("batch"),
            P("batch", None),
            P("batch"),
            P("batch"),
            P(),
            P("ens", None, None),
            P("ens", None),
        ),
        out_specs=(P("ens", "batch", None), P("ens", None), P("ens", None)),
        check_vma=False,
    )
```

```python
import functools

import jax
import jax.numpy as jnp
from jax import lax
from jax.experimental import pallas as pl
from jax.experimental.pallas import tpu as pltpu
from jax.sharding import PartitionSpec as P

discount = 0.99
entropy_temp = 0.2
penalty_weight = 1.0
diversity_weight = 1000.0

MESH = pl.DeviceIdType.MESH
F32 = jnp.float32
BF16 = jnp.bfloat16
CHUNK = 256
LANES = 128
VMEM_LIMIT = 36 * 1024 * 1024
VMEM_LIMIT_2 = 24 * 1024 * 1024


def dot_t(a, b):
    return lax.dot_general(a, b, (((1,), (1,)), ((), ())), preferred_element_type=F32)


def sigmoid(x):
    return 0.5 * jnp.tanh(0.5 * x) + 0.5


def kernel(
    n_ens, per_dev, samples, critics_total,
    rows_ref, next_act_ref, data_act_ref, samp_act_ref, reward_ref, logp_ref, w2_ref,
    obs_hbm, next_hbm, table_hbm, w1_ref,
    lhs_hbm, rhs_hbm, gv_ref, stat_ref,
    obs_ref, next_ref, table_ref, acts_ref, aux_ref, wbuf, xcat, xnext, acts_in, aux_in, sel, sel_dq, ptab,
    pbuf_a, pbuf_b, base, pcat, vb, cot, sbuf, ubuf,
    gpart, gsend, grecv, qpart, qrecv, unit, usend, urecv, qmine, qall, spread_mine, spread_all, spread,
    dgrad, dcoef_buf, gvsamp, gvbuf, lhs, tabd,
    in_sem, w_sem, a_send, a_recv, g_send, g_recv, u_send, u_recv, m_send, m_recv, s_send, s_recv,
    v_send, v_recv, o_sem, known,
):
    e = lax.axis_index("ens")
    b = lax.axis_index("batch")
    peer = 1 - b
    states = 2 * per_dev
    block = 2 * states
    nact = table_ref.shape[0]
    width = table_ref.shape[1]
    cols = acts_ref.shape[1]
    samp_cols = cols - block
    groups = samp_cols // LANES
    half = wbuf.shape[0]
    chunks = half // CHUNK
    pair = {"ens": e, "batch": peer}

    def other(k):
        return {"ens": lax.rem(e + k, n_ens), "batch": b}

    levels = n_ens.bit_length() - 1
    partners = []
    for k in range(levels):
        step = 1 << k
        partners.append({"ens": e + step * (1 - 2 * (lax.div(e, step) % 2)), "batch": b})
    partners.append(pair)
    barrier = pltpu.get_barrier_semaphore()
    for to in partners:
        pl.semaphore_signal(barrier, inc=1, device_id=to, device_id_type=MESH)

    def announce(k):
        pl.semaphore_signal(known.at[k], inc=1, device_id=partners[k], device_id_type=MESH)

    def advance(first_level, last_level):
        for k in range(first_level, last_level):
            pl.semaphore_wait(known.at[k], 1)
            announce(k + 1)

    quarter = -(-levels // 4)
    marks = [min(levels, quarter * k) for k in range(5)]
    loads = [
        pltpu.make_async_copy(obs_hbm, obs_ref, in_sem.at[0]),
        pltpu.make_async_copy(table_hbm, table_ref, in_sem.at[1]),
        pltpu.make_async_copy(next_hbm, next_ref, in_sem.at[2]),
    ]
    for copy in loads:
        copy.start()

    def w_copy(c):
        return pltpu.make_async_copy(
            w1_ref.at[0, pl.ds(b * half + c * CHUNK, CHUNK), :],
            wbuf.at[pl.ds(c * CHUNK, CHUNK), :],
            w_sem.at[c],
        )

    own_rows = pl.ds(pl.multiple_of(b * per_dev, per_dev), per_dev)
    peer_rows = pl.ds(pl.multiple_of(peer * per_dev, per_dev), per_dev)

    def one_hot(index_row, length):
        row = jnp.concatenate([index_row, jnp.zeros((1, LANES - per_dev), jnp.int32)], axis=1)
        hit = row == lax.broadcasted_iota(jnp.int32, (length, LANES), 0)
        return jnp.transpose(jnp.where(hit, 1.0, 0.0))[:per_dev, :].astype(BF16)

    pick = one_hot(rows_ref[...], obs_ref.shape[0])
    act_rows = [next_act_ref[...], data_act_ref[...]]
    act_rows += [samp_act_ref[i:i + 1, :] for i in range(samples)]

    def place(part):
        return [jnp.where(b == 0, part, jnp.zeros_like(part)), jnp.where(b == 0, jnp.zeros_like(part), part)]

    for j in range(cols // block):
        acts_ref[:, j * block:(j + 1) * block] = jnp.concatenate(
            place(act_rows[2 * j]) + place(act_rows[2 * j + 1]), axis=1
        )
    blank = jnp.zeros((1, states), F32)
    aux_ref[0:1, :] = jnp.concatenate([blank] + place(reward_ref[...]), axis=1)
    aux_ref[1:2, :] = jnp.concatenate([blank] + place(logp_ref[...]), axis=1)
    loads[0].wait()
    for c in range(chunks):
        w_copy(c).start()
    xcat[own_rows, :] = jnp.dot(pick, obs_ref[...], preferred_element_type=F32).astype(BF16)
    pl.semaphore_wait(barrier, len(partners))
    announce(0)

    def remote(src, dst, send, recv, to):
        return pltpu.make_async_remote_copy(
            src_ref=src, dst_ref=dst, send_sem=send, recv_sem=recv,
            device_id=to, device_id_type=MESH,
        )

    first = [
        remote(acts_ref, acts_in, a_send.at[0], a_recv.at[0], pair),
        remote(xcat.at[own_rows, :], xcat.at[own_rows, :], a_send.at[1], a_recv.at[1], pair),
        remote(xnext.at[own_rows, :], xnext.at[own_rows, :], a_send.at[2], a_recv.at[2], pair),
        remote(aux_ref, aux_in, a_send.at[3], a_recv.at[3], pair),
    ]
    first[0].start()
    first[1].start()
    loads[1].wait()
    moved = jnp.dot(one_hot(next_act_ref[...], nact), table_ref[...], preferred_element_type=F32)
    loads[2].wait()
    moved = moved + jnp.dot(pick, next_ref[...], preferred_element_type=F32)
    xnext[own_rows, :] = moved.astype(BF16)
    first[2].start()
    first[3].start()
    advance(marks[0], marks[1])

    def table_step(c, carry):
        rows = pl.ds(pl.multiple_of(c * CHUNK, CHUNK), CHUNK)
        w_copy(c).wait()
        ptab[rows, :] = (0.5 * dot_t(wbuf[rows, :], table_ref[...])).astype(BF16)
        v_row = w2_ref[0:1, pl.ds(pl.multiple_of(b * half + c * CHUNK, CHUNK), CHUNK)]
        vb[rows, :] = jnp.transpose(jnp.broadcast_to(v_row, (LANES, CHUNK)))
        return carry

    lax.fori_loop(0, chunks, table_step, 0)

    advance(marks[1], marks[2])
    first[0].wait()
    acts = acts_ref[...] + acts_in[...]
    hit = acts[:, :block] == lax.broadcasted_iota(jnp.int32, (nact, block), 0)
    picked = jnp.transpose(jnp.where(hit, 1.0, 0.0))[states:, :].astype(BF16)
    tabd[...] = jnp.dot(picked, table_ref[...], preferred_element_type=F32)
    advance(marks[2], marks[3])
    lane = lax.broadcasted_iota(jnp.int32, (1, block), 1)
    low = lane < states
    first[1].wait()
    xcat[states:, :] = (xcat[:states, :].astype(F32) + tabd[...]).astype(BF16)

    def chunk_rows(c):
        return slice(c * CHUNK, (c + 1) * CHUNK)

    def data_matmul(c):
        pcat[chunk_rows(c), :] = dot_t(wbuf[chunk_rows(c), :], xcat[...])

    def data_forward(c, q_acc):
        rows = chunk_rows(c)
        pre = pcat[rows, :]
        base[rows, :] = 0.5 * jnp.where(low, pre, pltpu.roll(pre, states, 1))
        v = vb[rows, :]
        sig = sigmoid(pre)
        silu = pre * sig
        weighted = v * (sig * (1.0 + (pre - silu)))
        lhs[rows, nact + block:] = jnp.where(low, 0.0, weighted).astype(BF16)
        cot[:, rows] = jnp.transpose(weighted)[states:, :].astype(BF16)
        return q_acc + jnp.sum(silu * v, axis=0, keepdims=True)

    q_data = jnp.zeros((1, block), F32)
    data_matmul(0)
    for c in range(chunks):
        if c + 1 < chunks:
            data_matmul(c + 1)
        q_data = data_forward(c, q_data)
    gpart[...] = jnp.dot(cot[...], wbuf[...], preferred_element_type=F32)
    gsend[...] = gpart[...].astype(BF16)
    qpart[:, :block] = q_data
    second = [
        remote(qpart.at[:, :block], qrecv.at[:, :block], g_send.at[0], g_recv.at[0], pair),
        remote(gsend.at[peer_rows, :], grecv.at[peer_rows, :], g_send.at[1], g_recv.at[1], pair),
        remote(qpart.at[:, block:], qrecv.at[:, block:], g_send.at[2], g_recv.at[2], pair),
        remote(gsend.at[own_rows, :], grecv.at[own_rows, :], g_send.at[3], g_recv.at[3], pair),
    ]
    second[1].start()
    advance(marks[3], marks[4])
    state_row = nact + lax.rem(lax.broadcasted_iota(jnp.int32, (1, LANES), 1), states)
    for j in range(groups):
        row = lax.broadcasted_iota(jnp.int32, (nact + block, LANES), 0)
        hit = jnp.logical_or(row == acts[:, block + j * LANES:block + (j + 1) * LANES], row == state_row)
        sel[:, j * LANES:(j + 1) * LANES] = jnp.where(hit, 1.0, 0.0).astype(BF16)

    first[2].wait()

    def next_forward(c, acc):
        rows = pl.ds(pl.multiple_of(c * 2 * CHUNK, 2 * CHUNK), 2 * CHUNK)
        pre = dot_t(wbuf[rows, :], xnext[...])
        silu = pre * sigmoid(pre)
        return acc + jnp.sum(silu * vb[rows, :states], axis=0, keepdims=True)

    q_next = lax.fori_loop(0, chunks // 2, next_forward, jnp.zeros((1, states), F32))
    qpart[:, :states] = q_next
    second[0].start()
    second[3].start()

    def samp_matmul(c, buf):
        rows = pl.ds(pl.multiple_of(c * CHUNK, CHUNK), CHUNK)
        buf[...] = jnp.dot(ptab[rows, :], sel[:nact, :], preferred_element_type=F32)

    SUB = 32

    def samp_forward(c, buf, q_acc):
        q_acc = list(q_acc)
        for r in range(CHUNK // SUB):
            here = slice(r * SUB, (r + 1) * SUB)
            there = pl.ds(pl.multiple_of(c * CHUNK + r * SUB, SUB), SUB)
            v = vb[there, :]
            start = base[there, :]
            for j in range(groups):
                at = slice(j * LANES, (j + 1) * LANES)
                h = buf[here, at] + start
                t = jnp.tanh(h)
                m = h * t
                silu = h + m
                slope = (1.0 + t) * (1.0 + (h - m))
                sbuf[there, at] = slope.astype(BF16)
                ubuf[there, at] = silu.astype(BF16)
                sv = silu * v
                part = sv[0:8]
                for i in range(1, SUB // 8):
                    part = part + sv[8 * i:8 * i + 8]
                q_acc[j] = q_acc[j] + part
        return tuple(q_acc)

    def samp_pair(k, q_acc):
        samp_matmul(2 * k + 1, pbuf_b)
        q_acc = samp_forward(2 * k, pbuf_a, q_acc)
        samp_matmul(lax.rem(2 * k + 2, chunks), pbuf_a)
        return samp_forward(2 * k + 1, pbuf_b, q_acc)

    q_acc = (jnp.zeros((8, LANES), F32),) * groups
    cut_one = chunks // 8
    samp_matmul(0, pbuf_a)
    q_acc = lax.fori_loop(0, cut_one, samp_pair, q_acc)

    def q_copy(k):
        return remote(qmine, qall.at[k], m_send.at[k], m_recv.at[k], other(k))

    def u_copy(k):
        return remote(
            usend.at[lax.rem(e + k, n_ens)], urecv.at[k], u_send.at[k], u_recv.at[k], other(k)
        )

    def s_copy(k):
        return remote(spread_mine, spread_all.at[b, e], s_send.at[0, k], s_recv.at[0, k], other(k))

    def s_cross(k):
        to = {"ens": lax.rem(e + k, n_ens), "batch": peer}
        return remote(spread_mine, spread_all.at[b, e], s_send.at[1, k], s_recv.at[1, k], to)

    def start_all(make, begin=1):
        def go(k, carry):
            make(k).start()
            return carry
        lax.fori_loop(begin, n_ens, go, 0)

    def wait_all(make, begin=1):
        def go(k, carry):
            make(k).wait()
            return carry
        lax.fori_loop(begin, n_ens, go, 0)

    second[1].wait()
    grad_in = gpart[own_rows, :] + grecv[own_rows, :].astype(F32)
    unit[...] = grad_in / jnp.sqrt(jnp.sum(grad_in * grad_in, axis=-1, keepdims=True) + 1.0)
    piece = usend.shape[1]
    per_col = per_dev // piece
    for p in range(n_ens):
        c0, r0 = p // per_col, (p % per_col) * piece
        usend[p] = unit[r0:r0 + piece, c0 * LANES:(c0 + 1) * LANES].astype(BF16)
    start_all(u_copy)
    second[0].wait()
    q0 = qpart[:, :block] + qrecv[:, :block]
    qmine[...] = jnp.broadcast_to(q0, qmine.shape)
    start_all(q_copy)

    q_acc = lax.fori_loop(cut_one, chunks // 2, samp_pair, q_acc)
    for j in range(groups):
        qpart[:, block + j * LANES:block + (j + 1) * LANES] = jnp.sum(q_acc[j], axis=0, keepdims=True)
    second[2].start()

    pl.semaphore_wait(known.at[levels], 1)
    wait_all(u_copy)
    total = usend[e].astype(F32)
    for k in range(1, n_ens):
        total = total + urecv[k].astype(F32)
    spread_mine[...] = total.astype(BF16)
    spread_all[b, e] = total.astype(BF16)
    start_all(s_cross, 0)
    start_all(s_copy)
    wait_all(q_copy)
    floor = qmine[...]
    for k in range(1, n_ens):
        floor = jnp.minimum(floor, qall[k])
    floor = pltpu.roll(floor, states, 1)[0:1, :]
    first[3].wait()
    aux = aux_ref[...] + aux_in[...]
    target = aux[0:1, :] + discount * (floor - entropy_temp * aux[1:2, :])
    td_gap = q0 - target
    dq_data = jnp.where(low, 0.0, (2.0 * td_gap - penalty_weight) / states)

    second[2].wait()
    q_samp = qpart[:, block:] + qrecv[:, block:]
    exps = jnp.exp(q_samp)
    mass = exps[:, :block]
    for j in range(1, groups):
        mass = mass + exps[:, j * block:(j + 1) * block]
    mass = mass + pltpu.roll(mass, states, 1)
    log_mass = jnp.log(mass)
    tiled = jnp.concatenate([log_mass] * groups, axis=1)
    dq_samp = penalty_weight * jnp.exp(q_samp - tiled) / states
    for j in range(groups):
        at = slice(j * LANES, (j + 1) * LANES)
        sel_dq[:, at] = (sel[:, at].astype(F32) * (0.5 * dq_samp[:, at])).astype(BF16)

    def samp_gv(c, carry):
        there = pl.ds(pl.multiple_of(c * SUB * 2, SUB * 2), SUB * 2)
        total = ubuf[there, :LANES].astype(F32) * dq_samp[:, :LANES]
        for j in range(1, groups):
            at = slice(j * LANES, (j + 1) * LANES)
            total = total + ubuf[there, at].astype(F32) * dq_samp[:, at]
        gvsamp[there, :] = total
        return carry

    def samp_step(c, carry):
        rows = pl.ds(pl.multiple_of(c * 2 * CHUNK, 2 * CHUNK), 2 * CHUNK)
        grads = dot_t(sbuf[rows, :], sel_dq[...])
        v = vb[rows, :]
        for j in range((nact + block) // LANES):
            at = slice(j * LANES, (j + 1) * LANES)
            lhs[rows, at] = (v * grads[:, at]).astype(BF16)
        return carry

    lax.fori_loop(0, half // (SUB * 2), samp_gv, 0)
    steps = chunks // 2
    lax.fori_loop(0, steps // 2, samp_step, 0)
    second[3].wait()
    grad_in = gpart[...] + grecv[...].astype(F32)
    in_norm = jnp.sqrt(jnp.sum(grad_in * grad_in, axis=-1, keepdims=True) + 1.0)
    unit_dir = grad_in / in_norm
    wait_all(s_cross, 0)
    wait_all(s_copy)
    scale = 2.0 * diversity_weight / (critics_total - 1) / states
    for i in range(2):
        for p in range(n_ens):
            c0, r0 = p // per_col, i * per_dev + (p % per_col) * piece
            spread[r0:r0 + piece, c0 * LANES:(c0 + 1) * LANES] = spread_all[i, p].astype(F32)
    away = spread[...] - unit_dir
    div_row = jnp.sum(unit_dir * away, axis=-1, keepdims=True)
    dgrad[:states, :] = jnp.zeros((states, width), BF16)
    dgrad[states:, :] = (scale * (away - unit_dir * div_row) / in_norm).astype(BF16)
    rhs_out = [
        pltpu.make_async_copy(table_ref, rhs_hbm.at[:nact], in_sem.at[0]),
        pltpu.make_async_copy(xcat, rhs_hbm.at[nact:nact + block], in_sem.at[1]),
        pltpu.make_async_copy(dgrad, rhs_hbm.at[nact + block:], in_sem.at[2]),
    ]
    for copy in rhs_out:
        copy.start()

    def dcoef_matmul(c):
        dcoef_buf[chunk_rows(c), :] = dot_t(wbuf[chunk_rows(c), :], dgrad[...])

    def data_backward(c):
        rows = chunk_rows(c)
        dcoef = dcoef_buf[rows, :]
        pre = pcat[rows, :]
        v = vb[rows, :]
        sig = sigmoid(pre)
        silu = pre * sig
        slope = sig * (1.0 + (pre - silu))
        curve = sig * (1.0 - sig) * (2.0 + pre * (1.0 - 2.0 * sig))
        dcoef_buf[rows, :] = v * (dq_data * slope + dcoef * curve)
        gv = gvsamp[rows, :] + jnp.where(low, 0.0, dq_data * silu + dcoef * slope)
        gvbuf[b, c:c + 1, :] = jnp.sum(jnp.transpose(gv), axis=0, keepdims=True)

    dcoef_matmul(0)
    for c in range(chunks):
        if c + 1 < chunks:
            dcoef_matmul(c + 1)
        data_backward(c)
    last = remote(gvbuf.at[b], gvbuf.at[b], v_send, v_recv, pair)
    last.start()
    lax.fori_loop(steps // 2, steps, samp_step, 0)

    def lhs_copy(c):
        rows = pl.ds(c * CHUNK, CHUNK)
        return pltpu.make_async_copy(lhs.at[rows, :], lhs_hbm.at[rows, :], o_sem.at[c])

    mid = slice(nact, nact + block)
    for c in range(chunks):
        rows = chunk_rows(c)
        lhs[rows, mid] = jnp.where(low, lhs[rows, mid].astype(F32), dcoef_buf[rows, :]).astype(BF16)
        lhs_copy(c).start()

    td_total = jnp.sum(jnp.where(low, 0.0, td_gap * td_gap), axis=1, keepdims=True)
    gap_total = jnp.sum(jnp.where(low, 0.0, log_mass - q0), axis=1, keepdims=True)
    div_total = jnp.sum(div_row, axis=0, keepdims=True)
    stats = jnp.where(lane == 0, td_total, jnp.where(lane == 1, gap_total, div_total))
    stat_ref[...] = (stats / states)[:, :3]
    last.wait()
    for i in range(2):
        for c in range(chunks):
            at = i * half + c * CHUNK
            gv_ref[:, at:at + CHUNK] = gvbuf[i, c:c + 1, :]
    for copy in rhs_out:
        copy.wait()
    for c in range(chunks):
        lhs_copy(c).wait()


def finish(lhs_ref, rhs_ref, gv_ref, stat_ref, out_hbm, gv_out, stat_out, buf, sem):
    gv_out[...] = gv_ref[...]
    stat_out[...] = stat_ref[...]
    parts = 4
    tile = buf.shape[0] // parts
    copies = []
    for i in range(parts):
        rows = pl.ds(i * tile, tile)
        buf[rows, :] = jnp.dot(lhs_ref[rows, :], rhs_ref[...], preferred_element_type=F32)
        copies.append(pltpu.make_async_copy(buf.at[rows, :], out_hbm.at[0, rows, :], sem.at[i]))
        copies[-1].start()
    for copy in copies:
        copy.wait()


def body(
    replay_obs, replay_next, batch_rows, data_action, next_action, sampled_actions,
    reward, next_logp, action_table, w1, w2,
):
    per_dev = batch_rows.shape[0]
    samples = sampled_actions.shape[1]
    width = replay_obs.shape[1]
    hidden = w1.shape[1]
    n_batch = lax.axis_size("batch")
    n_ens = lax.axis_size("ens")
    if n_batch != 2 or w1.shape[0] != 1 or n_ens & (n_ens - 1):
        raise ValueError("unsupported mesh")
    states = per_dev * n_batch
    block = 2 * states
    half = hidden // n_batch
    nact = action_table.shape[0]
    cols = (samples + 2) * states
    samp_cols = cols - block
    inner = nact + 2 * block
    chunks = half // CHUNK
    piece = per_dev * width // LANES // n_ens
    vmem = pl.BlockSpec(memory_space=pltpu.VMEM)
    anywhere = pl.BlockSpec(memory_space=pl.ANY)
    hbm = pl.BlockSpec(memory_space=pltpu.HBM)
    dma = pltpu.SemaphoreType.DMA
    lhs, rhs, gv, stats = pl.pallas_call(
        functools.partial(kernel, n_ens, per_dev, samples, n_ens * w1.shape[0]),
        out_shape=(
            jax.ShapeDtypeStruct((half, inner), BF16),
            jax.ShapeDtypeStruct((inner, width), BF16),
            jax.ShapeDtypeStruct((1, hidden), F32),
            jax.ShapeDtypeStruct((1, 3), F32),
        ),
        in_specs=[vmem] * 7 + [hbm] * 4,
        out_specs=(anywhere, anywhere, vmem, vmem),
        scratch_shapes=[
            pltpu.VMEM(replay_obs.shape, BF16),
            pltpu.VMEM(replay_next.shape, BF16),
            pltpu.VMEM(action_table.shape, BF16),
            pltpu.VMEM((1, cols), jnp.int32),
            pltpu.VMEM((2, block), F32),
            pltpu.VMEM((half, width), BF16),
            pltpu.VMEM((block, width), BF16),
            pltpu.VMEM((states, width), BF16),
            pltpu.VMEM((1, cols), jnp.int32),
            pltpu.VMEM((2, block), F32),
            pltpu.VMEM((nact + block, samp_cols), BF16),
            pltpu.VMEM((nact + block, samp_cols), BF16),
            pltpu.VMEM((half, nact), BF16),
            pltpu.VMEM((CHUNK, samp_cols), F32),
            pltpu.VMEM((CHUNK, samp_cols), F32),
            pltpu.VMEM((half, block), F32),
            pltpu.VMEM((half, block), F32),
            pltpu.VMEM((half, LANES), F32),
            pltpu.VMEM((states, half), BF16),
            pltpu.VMEM((half, samp_cols), BF16),
            pltpu.VMEM((half, samp_cols), BF16),
            pltpu.VMEM((states, width), F32),
            pltpu.VMEM((states, width), BF16),
            pltpu.VMEM((states, width), BF16),
            pltpu.VMEM((1, cols), F32),
            pltpu.VMEM((1, cols), F32),
            pltpu.VMEM((per_dev, width), F32),
            pltpu.VMEM((n_ens, piece, LANES), BF16),
            pltpu.VMEM((n_ens, piece, LANES), BF16),
            pltpu.VMEM((8, block), F32),
            pltpu.VMEM((n_ens, 8, block), F32),
            pltpu.VMEM((piece, LANES), BF16),
            pltpu.VMEM((2, n_ens, piece, LANES), BF16),
            pltpu.VMEM((states, width), F32),
            pltpu.VMEM((block, width), BF16),
            pltpu.VMEM((half, block), F32),
            pltpu.VMEM((half, LANES), F32),
            pltpu.VMEM((2, chunks, CHUNK), F32),
            pltpu.VMEM((half, inner), BF16),
            pltpu.VMEM((states, width), F32),
            dma((3,)), dma((chunks,)),
            dma((4,)), dma((4,)), dma((4,)), dma((4,)),
            dma((n_ens,)), dma((n_ens,)), dma((n_ens,)), dma((n_ens,)), dma((2, n_ens)), dma((2, n_ens)),
            dma, dma, dma((chunks,)), pltpu.SemaphoreType.REGULAR((n_ens.bit_length(),)),
        ],
        compiler_params=pltpu.CompilerParams(
            collective_id=0, has_side_effects=True, vmem_limit_bytes=VMEM_LIMIT
        ),
    )(*(
        pltpu.with_memory_space_constraint(x, pltpu.HBM)
        for x in (
            batch_rows[None], next_action[None], data_action[None],
            sampled_actions.T, reward[None], next_logp[None], w2,
            replay_obs, replay_next, action_table, w1,
        )
    ))
    return pl.pallas_call(
        finish,
        out_shape=(
            jax.ShapeDtypeStruct((1, half, width), F32),
            jax.ShapeDtypeStruct((1, hidden), F32),
            jax.ShapeDtypeStruct((1, 3), F32),
        ),
        in_specs=[vmem] * 4,
        out_specs=(hbm, vmem, vmem),
        scratch_shapes=[pltpu.VMEM((half, width), F32), dma((4,))],
        compiler_params=pltpu.CompilerParams(vmem_limit_bytes=VMEM_LIMIT_2),
    )(lhs, rhs, gv, stats)


def solution(mesh):
    return jax.shard_map(
        body,
        mesh=mesh,
        in_specs=(
            P("batch", None),
            P("batch", None),
            P("batch"),
            P("batch"),
            P("batch"),
            P("batch", None),
            P("batch"),
            P("batch"),
            P(),
            P("ens", None, None),
            P("ens", None),
        ),
        out_specs=(P("ens", "batch", None), P("ens", None), P("ens", None)),
        check_vma=False,
    )
```

```python
import functools

import jax
import jax.numpy as jnp
from jax import lax
from jax.experimental import pallas as pl
from jax.experimental.pallas import tpu as pltpu
from jax.sharding import PartitionSpec as P

discount = 0.99
entropy_temp = 0.2
penalty_weight = 1.0
diversity_weight = 1000.0

MESH = pl.DeviceIdType.MESH
F32 = jnp.float32
BF16 = jnp.bfloat16
CHUNK = 256
LANES = 128
VMEM_LIMIT = 36 * 1024 * 1024
VMEM_LIMIT_2 = 24 * 1024 * 1024


def dot_t(a, b):
    return lax.dot_general(a, b, (((1,), (1,)), ((), ())), preferred_element_type=F32)


def sigmoid(x):
    return 0.5 * jnp.tanh(0.5 * x) + 0.5


def kernel(
    n_ens, per_dev, samples, critics_total,
    rows_ref, next_act_ref, data_act_ref, samp_act_ref, reward_ref, logp_ref, w2_ref,
    obs_hbm, next_hbm, table_hbm, w1_ref,
    lhs, rhs, gv_ref, stat_ref,
    obs_ref, next_ref, table_ref, acts_ref, aux_ref, wbuf, xobs, xnext, xdat, xin, xnx, acts_in, aux_in, sel, sel_dq, ptab,
    pbuf_a, pbuf_b, base, pcat, vb, cot, sbuf, ubuf,
    gpart, gsend, grecv, qpart, qrecv, unit, usend, urecv, qmine, qall, spread_mine, spread_all, spread,
    dcoef_buf, gvsamp, tabd,
    in_sem, w_sem, a_send, a_recv, g_send, g_recv, u_send, u_recv, m_send, m_recv, s_send, s_recv,
    known,
):
    e = lax.axis_index("ens")
    b = lax.axis_index("batch")
    peer = 1 - b
    states = 2 * per_dev
    block = 2 * states
    nact = table_ref.shape[0]
    width = table_ref.shape[1]
    cols = acts_ref.shape[1]
    samp_cols = cols - block
    groups = samp_cols // LANES
    half = wbuf.shape[0]
    chunks = half // CHUNK
    pairs = chunks // 2
    pair = {"ens": e, "batch": peer}

    def other(k):
        return {"ens": lax.rem(e + k, n_ens), "batch": b}

    levels = n_ens.bit_length() - 1
    cube = levels - 1
    line = n_ens // 4
    z = lax.div(e, line)
    middle = jnp.logical_and(z >= 1, z <= 2)

    def at_ens(k):
        return {"ens": k, "batch": b}

    partners = [at_ens(e + (1 << k) * (1 - 2 * (lax.div(e, 1 << k) % 2))) for k in range(cube)]
    across = at_ens(e + line * (3 - 2 * z))
    barrier = pltpu.get_barrier_semaphore()
    for to in partners + [pair]:
        pl.semaphore_signal(barrier, inc=1, device_id=to, device_id_type=MESH)

    @pl.when(middle)
    def greet_across():
        pl.semaphore_signal(barrier, inc=1, device_id=across, device_id_type=MESH)

    def tell(k, to):
        pl.semaphore_signal(known.at[k], inc=1, device_id=to, device_id_type=MESH)

    def hear(k):
        pl.semaphore_wait(known.at[k], 1)

    def advance(first_level, last_level):
        for k in range(first_level, last_level):
            hear(k)
            if k + 1 < cube:
                tell(k + 1, partners[k + 1])

    def cross_tell():
        @pl.when(middle)
        def go():
            tell(cube, across)

    def cross_hear():
        @pl.when(middle)
        def go():
            hear(cube)
            tell(cube + 1, partners[cube - 1])

    def edge_hear():
        @pl.when(jnp.logical_not(middle))
        def go():
            hear(cube + 1)

        tell(cube + 2, pair)

    third = -(-cube // 3)
    marks = [min(cube, third * k) for k in range(4)]
    loads = [
        pltpu.make_async_copy(obs_hbm, obs_ref, in_sem.at[0]),
        pltpu.make_async_copy(table_hbm, table_ref, in_sem.at[1]),
        pltpu.make_async_copy(next_hbm, next_ref, in_sem.at[2]),
    ]
    for copy in loads:
        copy.start()

    def w_copy(c):
        return pltpu.make_async_copy(
            w1_ref.at[0, pl.ds(b * half + c * CHUNK, CHUNK), :],
            wbuf.at[pl.ds(c * CHUNK, CHUNK), :],
            w_sem.at[c],
        )

    d_top = nact + 3 * states
    own_rows = pl.ds(pl.multiple_of(b * per_dev, per_dev), per_dev)
    peer_rows = pl.ds(pl.multiple_of(peer * per_dev, per_dev), per_dev)

    def one_hot(index_row, length):
        row = jnp.concatenate([index_row, jnp.zeros((1, LANES - per_dev), jnp.int32)], axis=1)
        hit = row == lax.broadcasted_iota(jnp.int32, (length, LANES), 0)
        return jnp.transpose(jnp.where(hit, 1.0, 0.0))[:per_dev, :].astype(BF16)

    pick = one_hot(rows_ref[...], obs_ref.shape[0])
    act_rows = [next_act_ref[...], data_act_ref[...]]
    act_rows += [samp_act_ref[i:i + 1, :] for i in range(samples)]

    def place(part):
        return [jnp.where(b == 0, part, jnp.zeros_like(part)), jnp.where(b == 0, jnp.zeros_like(part), part)]

    for j in range(cols // block):
        acts_ref[:, j * block:(j + 1) * block] = jnp.concatenate(
            place(act_rows[2 * j]) + place(act_rows[2 * j + 1]), axis=1
        )
    aux_ref[0:1, :] = jnp.concatenate(place(reward_ref[...]) * 2, axis=1)
    aux_ref[1:2, :] = jnp.concatenate(place(logp_ref[...]) * 2, axis=1)
    for c in range(chunks):
        w_copy(c).start()
    for g in range(pairs):
        v_row = w2_ref[0:1, pl.ds(pl.multiple_of(b * half + 2 * g * CHUNK, CHUNK), 2 * CHUNK)]
        vb[2 * g * CHUNK:2 * (g + 1) * CHUNK, :] = jnp.transpose(jnp.broadcast_to(v_row, (LANES, 2 * CHUNK)))
    for i in range(2):
        gap = slice((1 - i) * states, (2 - i) * states)
        xin[i, gap, :] = jnp.zeros((states, width), BF16)
        xnx[i, gap, :] = jnp.zeros((states, width), BF16)
        rhs[d_top + 2 * i * states:d_top + (2 * i + 1) * states, :] = jnp.zeros((states, width), BF16)
    loads[0].wait()
    xobs[own_rows, :] = jnp.dot(pick, obs_ref[...], preferred_element_type=F32).astype(BF16)
    pl.semaphore_wait(barrier, len(partners) + 1 + jnp.where(middle, 1, 0))
    tell(0, partners[0])

    def remote(src, dst, send, recv, to):
        return pltpu.make_async_remote_copy(
            src_ref=src, dst_ref=dst, send_sem=send, recv_sem=recv,
            device_id=to, device_id_type=MESH,
        )

    first = [
        remote(acts_ref, acts_in, a_send.at[0], a_recv.at[0], pair),
        remote(xobs.at[own_rows, :], xobs.at[own_rows, :], a_send.at[1], a_recv.at[1], pair),
        remote(xnext.at[own_rows, :], xnext.at[own_rows, :], a_send.at[2], a_recv.at[2], pair),
        remote(aux_ref, aux_in, a_send.at[3], a_recv.at[3], pair),
    ]
    first[0].start()
    first[1].start()
    loads[1].wait()
    moved = jnp.dot(one_hot(next_act_ref[...], nact), table_ref[...], preferred_element_type=F32)
    loads[2].wait()
    moved = moved + jnp.dot(pick, next_ref[...], preferred_element_type=F32)
    xnext[own_rows, :] = moved.astype(BF16)
    first[2].start()
    first[3].start()
    advance(marks[0], marks[1])

    for g in range(pairs):
        w_copy(2 * g).wait()
        w_copy(2 * g + 1).wait()
        rows = [slice((2 * g + i) * CHUNK, (2 * g + i + 1) * CHUNK) for i in range(2)]
        made = [dot_t(wbuf[r, :], table_ref[...]) for r in rows]
        for r, out in zip(rows, made):
            ptab[r, :] = (0.5 * out).astype(BF16)

    advance(marks[1], marks[2])
    first[0].wait()
    acts = acts_ref[...] + acts_in[...]
    hit = acts[:, :block] == lax.broadcasted_iota(jnp.int32, (nact, block), 0)
    picked = jnp.transpose(jnp.where(hit, 1.0, 0.0))[states:, :].astype(BF16)
    tabd[...] = jnp.dot(picked, table_ref[...], preferred_element_type=F32)
    advance(marks[2], marks[3])
    cross_tell()
    lane = lax.broadcasted_iota(jnp.int32, (1, block), 1)
    low = lane < states
    first[1].wait()
    obs_rows = xobs[...]
    data_rows = (obs_rows.astype(F32) + tabd[...]).astype(BF16)
    xdat[...] = data_rows
    for i in range(2):
        xin[i, i * states:(i + 1) * states, :] = data_rows
        xin[i, block:block + states, :] = obs_rows
        xin[i, block + states:, :] = obs_rows

    def chunk_rows(c):
        return slice(c * CHUNK, (c + 1) * CHUNK)

    def both(k, lhs_pair):
        one = dot_t(wbuf[chunk_rows(k), :], lhs_pair[0][...])
        two = dot_t(wbuf[chunk_rows(k + pairs), :], lhs_pair[1][...])
        return one, two

    def both_v(k):
        return jnp.where(low, vb[chunk_rows(k), :], vb[chunk_rows(k + pairs), :])

    def data_matmul(k):
        one, two = both(k, (xin.at[0], xin.at[1]))
        pcat[chunk_rows(k), :] = one[:, :block] + two[:, :block]
        base[chunk_rows(k), :] = 0.5 * one[:, block:]
        base[chunk_rows(k + pairs), :] = 0.5 * two[:, block:]

    def data_forward(k, q_acc):
        pre = pcat[chunk_rows(k), :]
        v = both_v(k)
        sig = sigmoid(pre)
        silu = pre * sig
        weighted = v * (sig * (1.0 + (pre - silu)))
        flat = jnp.transpose(weighted)
        for i in range(2):
            rows = chunk_rows(k + i * pairs)
            lhs[rows, nact + block:] = weighted.astype(BF16)
            cot[:, rows] = flat[i * states:(i + 1) * states, :].astype(BF16)
        return q_acc + jnp.sum(silu * v, axis=0, keepdims=True)

    q_data = jnp.zeros((1, block), F32)
    data_matmul(0)
    for k in range(pairs):
        if k + 1 < pairs:
            data_matmul(k + 1)
        q_data = data_forward(k, q_data)
    q_data = q_data + pltpu.roll(q_data, states, 1)
    gpart[...] = jnp.dot(cot[...], wbuf[...], preferred_element_type=F32)
    gsend[...] = gpart[...].astype(BF16)
    second = [
        remote(qpart.at[:, :block], qrecv.at[:, :block], g_send.at[0], g_recv.at[0], pair),
        remote(gsend.at[peer_rows, :], grecv.at[peer_rows, :], g_send.at[1], g_recv.at[1], pair),
        remote(qpart.at[:, block:], qrecv.at[:, block:], g_send.at[2], g_recv.at[2], pair),
        remote(gsend.at[own_rows, :], grecv.at[own_rows, :], g_send.at[3], g_recv.at[3], pair),
    ]
    second[1].start()
    cross_hear()
    row = lax.broadcasted_iota(jnp.int32, (nact + block, LANES), 0)
    own_state = lax.rem(lax.broadcasted_iota(jnp.int32, (nact + block, LANES), 1), states)
    own_state = jnp.logical_and(row >= nact, lax.rem(row - nact, states) == own_state)
    for j in range(groups):
        hit = jnp.logical_or(row == acts[:, block + j * LANES:block + (j + 1) * LANES], own_state)
        sel[:, j * LANES:(j + 1) * LANES] = jnp.where(hit, 1.0, 0.0).astype(BF16)

    rhs[:nact, :] = table_ref[...]
    rhs[nact:nact + states, :] = xdat[...]
    rhs[nact + states:nact + block, :] = xobs[...]
    rhs[nact + block:d_top, :] = xdat[...]

    first[2].wait()
    for i in range(2):
        xnx[i, i * states:(i + 1) * states, :] = xnext[...]

    def next_matmul(k):
        one, two = both(k, (xnx.at[0], xnx.at[1]))
        dcoef_buf[chunk_rows(k), :] = one + two

    q_next = jnp.zeros((1, block), F32)
    next_matmul(0)
    for k in range(pairs):
        if k + 1 < pairs:
            next_matmul(k + 1)
        pre = dcoef_buf[chunk_rows(k), :]
        q_next = q_next + jnp.sum(pre * sigmoid(pre) * both_v(k), axis=0, keepdims=True)
    q_next = q_next + pltpu.roll(q_next, states, 1)
    qpart[:, :block] = jnp.where(low, q_next, q_data)
    second[0].start()
    second[3].start()

    def samp_matmul(c, buf):
        rows = pl.ds(pl.multiple_of(c * CHUNK, CHUNK), CHUNK)
        buf[...] = jnp.dot(ptab[rows, :], sel[:nact, :], preferred_element_type=F32)

    SUB = 32

    def samp_forward(c, buf, q_acc):
        q_acc = list(q_acc)
        for r in range(CHUNK // SUB):
            here = slice(r * SUB, (r + 1) * SUB)
            there = pl.ds(pl.multiple_of(c * CHUNK + r * SUB, SUB), SUB)
            v = vb[there, :]
            start = base[there, :]
            for j in range(groups):
                at = slice(j * LANES, (j + 1) * LANES)
                h = buf[here, at] + start
                t = jnp.tanh(h)
                m = h * t
                silu = h + m
                slope = (1.0 + t) * (1.0 + (h - m))
                sbuf[there, at] = slope.astype(BF16)
                ubuf[there, at] = silu.astype(BF16)
                sv = silu * v
                part = sv[0:8]
                for i in range(1, SUB // 8):
                    part = part + sv[8 * i:8 * i + 8]
                q_acc[j] = q_acc[j] + part
        return tuple(q_acc)

    def samp_pair(k, q_acc):
        samp_matmul(2 * k + 1, pbuf_b)
        q_acc = samp_forward(2 * k, pbuf_a, q_acc)
        samp_matmul(lax.rem(2 * k + 2, chunks), pbuf_a)
        return samp_forward(2 * k + 1, pbuf_b, q_acc)

    q_acc = (jnp.zeros((8, LANES), F32),) * groups
    cut_one = chunks // 8

    def q_copy(k):
        return remote(qmine, qall.at[k], m_send.at[k], m_recv.at[k], other(k))

    def u_copy(k):
        return remote(
            usend.at[lax.rem(e + k, n_ens)], urecv.at[k], u_send.at[k], u_recv.at[k], other(k)
        )

    def s_copy(k):
        return remote(spread_mine, spread_all.at[b, e], s_send.at[0, k], s_recv.at[0, k], other(k))

    def s_cross(k):
        to = {"ens": lax.rem(e + k, n_ens), "batch": peer}
        return remote(spread_mine, spread_all.at[b, e], s_send.at[1, k], s_recv.at[1, k], to)

    def start_all(make, begin=1):
        def go(k, carry):
            make(k).start()
            return carry
        lax.fori_loop(begin, n_ens, go, 0)

    def wait_all(make, begin=1):
        def go(k, carry):
            make(k).wait()
            return carry
        lax.fori_loop(begin, n_ens, go, 0)

    second[1].wait()
    grad_in = gpart[own_rows, :] + grecv[own_rows, :].astype(F32)
    edge_hear()
    unit[...] = grad_in / jnp.sqrt(jnp.sum(grad_in * grad_in, axis=-1, keepdims=True) + 1.0)
    piece = usend.shape[1]
    per_col = per_dev // piece
    for p in range(n_ens):
        c0, r0 = p // per_col, (p % per_col) * piece
        usend[p] = unit[r0:r0 + piece, c0 * LANES:(c0 + 1) * LANES].astype(BF16)
    start_all(u_copy)
    samp_matmul(0, pbuf_a)
    q_acc = lax.fori_loop(0, cut_one, samp_pair, q_acc)
    second[0].wait()
    q0 = qpart[:, :block] + qrecv[:, :block]
    qmine[...] = jnp.broadcast_to(q0, qmine.shape)
    start_all(q_copy)

    q_acc = lax.fori_loop(cut_one, chunks // 2, samp_pair, q_acc)
    for j in range(groups):
        qpart[:, block + j * LANES:block + (j + 1) * LANES] = jnp.sum(q_acc[j], axis=0, keepdims=True)
    second[2].start()

    hear(cube + 2)
    wait_all(u_copy)
    total = usend[e].astype(F32)
    for k in range(1, n_ens):
        total = total + urecv[k].astype(F32)
    spread_mine[...] = total.astype(BF16)
    spread_all[b, e] = total.astype(BF16)
    start_all(s_cross, 0)
    start_all(s_copy)
    wait_all(q_copy)
    floor = qmine[...]
    for k in range(1, n_ens):
        floor = jnp.minimum(floor, qall[k])
    floor = floor[0:1, :]
    floor = jnp.where(low, floor, pltpu.roll(floor, states, 1))
    q_own = jnp.where(low, pltpu.roll(q0, states, 1), q0)
    first[3].wait()
    aux = aux_ref[...] + aux_in[...]
    target = aux[0:1, :] + discount * (floor - entropy_temp * aux[1:2, :])
    td_gap = q_own - target
    dq_data = (2.0 * td_gap - penalty_weight) / states

    second[2].wait()
    q_samp = qpart[:, block:] + qrecv[:, block:]
    exps = jnp.exp(q_samp)
    mass = exps[:, :block]
    for j in range(1, groups):
        mass = mass + exps[:, j * block:(j + 1) * block]
    mass = mass + pltpu.roll(mass, states, 1)
    log_mass = jnp.log(mass)
    tiled = jnp.concatenate([log_mass] * groups, axis=1)
    dq_samp = penalty_weight * jnp.exp(q_samp - tiled) / states
    for j in range(groups):
        at = slice(j * LANES, (j + 1) * LANES)
        sel_dq[:, at] = (sel[:, at].astype(F32) * (0.5 * dq_samp[:, at])).astype(BF16)

    def samp_gv(c):
        there = slice(c * LANES, (c + 1) * LANES)
        total = ubuf[there, :LANES].astype(F32) * dq_samp[:, :LANES]
        for j in range(1, groups):
            at = slice(j * LANES, (j + 1) * LANES)
            total = total + ubuf[there, at].astype(F32) * dq_samp[:, at]
        gvsamp[:, there] = jnp.sum(jnp.transpose(total), axis=0, keepdims=True)

    mid = slice(nact, nact + block)

    def samp_step(k):
        rows = slice(k * 2 * CHUNK, (k + 1) * 2 * CHUNK)
        grads = dot_t(sbuf[rows, :], sel_dq[...])
        v = vb[rows, :]
        for j in range(nact // LANES):
            at = slice(j * LANES, (j + 1) * LANES)
            lhs[rows, at] = (v * grads[:, at]).astype(BF16)
        lhs[rows, mid] = (v * grads[:, mid]).astype(BF16)

    steps = chunks // 2
    share = half // LANES // steps
    for k in range(steps):
        samp_step(k)
        for c in range(k * share, (k + 1) * share):
            samp_gv(c)
    second[3].wait()
    grad_in = gpart[...] + grecv[...].astype(F32)
    in_norm = jnp.sqrt(jnp.sum(grad_in * grad_in, axis=-1, keepdims=True) + 1.0)
    unit_dir = grad_in / in_norm
    wait_all(s_cross, 0)
    wait_all(s_copy)
    scale = 2.0 * diversity_weight / (critics_total - 1) / states
    for i in range(2):
        for p in range(n_ens):
            c0, r0 = p // per_col, i * per_dev + (p % per_col) * piece
            spread[r0:r0 + piece, c0 * LANES:(c0 + 1) * LANES] = spread_all[i, p].astype(F32)
    away = spread[...] - unit_dir
    div_row = jnp.sum(unit_dir * away, axis=-1, keepdims=True)
    dgrad_rows = (scale * (away - unit_dir * div_row) / in_norm).astype(BF16)
    rhs[d_top + states:d_top + 2 * states, :] = dgrad_rows
    shifted = (rhs.at[d_top + states:, :], rhs.at[d_top:d_top + block, :])

    def dcoef_matmul(k):
        one, two = both(k, shifted)
        dcoef_buf[chunk_rows(k), :] = one + two

    def data_backward(k):
        dcoef = dcoef_buf[chunk_rows(k), :]
        pre = pcat[chunk_rows(k), :]
        v = both_v(k)
        sig = sigmoid(pre)
        silu = pre * sig
        slope = sig * (1.0 + (pre - silu))
        curve = sig * (1.0 - sig) * (2.0 + pre * (1.0 - 2.0 * sig))
        dpre = v * (dq_data * slope + dcoef * curve)
        rows = chunk_rows(k)
        lhs[rows, mid] = jnp.where(low, dpre, lhs[rows, mid].astype(F32)).astype(BF16)
        rows = chunk_rows(k + pairs)
        lhs[rows, mid] = jnp.where(low, lhs[rows, mid].astype(F32), dpre).astype(BF16)
        flat = jnp.transpose(dq_data * silu + dcoef * slope)
        for i in range(2):
            c = k + i * pairs
            late = jnp.sum(flat[i * states:(i + 1) * states, :], axis=0, keepdims=True)
            gv_ref[:, chunk_rows(c)] = gvsamp[:, chunk_rows(c)] + late

    dcoef_matmul(0)
    for k in range(pairs):
        if k + 1 < pairs:
            dcoef_matmul(k + 1)
        data_backward(k)
    td_total = jnp.sum(jnp.where(low, td_gap * td_gap, 0.0), axis=1, keepdims=True)
    gap_total = jnp.sum(jnp.where(low, log_mass - q_own, 0.0), axis=1, keepdims=True)
    div_total = jnp.sum(div_row, axis=0, keepdims=True)
    stats = jnp.where(lane == 0, td_total, jnp.where(lane == 1, gap_total, div_total))
    stat_ref[...] = (stats / states)[:, :3]


def finish(nact, lhs_ref, rhs_ref, stat_ref, out_hbm, stat_out, buf, sem):
    stat_out[...] = stat_ref[...]
    parts = sem.shape[0]
    tile = buf.shape[0] // parts
    states = (lhs_ref.shape[1] - nact) // 4
    block = 2 * states
    mids = []
    for i in range(2):
        x_top = nact + i * states
        d_top = nact + block + (2 - i) * states
        mids.append(jnp.concatenate([rhs_ref[x_top:x_top + block, :], rhs_ref[d_top:d_top + block, :]], axis=0))
    copies = []
    for i in range(parts):
        rows = pl.ds(i * tile, tile)
        out = jnp.dot(lhs_ref[rows, :nact], rhs_ref[:nact, :], preferred_element_type=F32)
        out += jnp.dot(lhs_ref[rows, nact:], mids[2 * i // parts], preferred_element_type=F32)
        buf[rows, :] = out
        copies.append(pltpu.make_async_copy(buf.at[rows, :], out_hbm.at[0, rows, :], sem.at[i]))
        copies[-1].start()
    for copy in copies:
        copy.wait()


def body(
    replay_obs, replay_next, batch_rows, data_action, next_action, sampled_actions,
    reward, next_logp, action_table, w1, w2,
):
    per_dev = batch_rows.shape[0]
    samples = sampled_actions.shape[1]
    width = replay_obs.shape[1]
    hidden = w1.shape[1]
    n_batch = lax.axis_size("batch")
    n_ens = lax.axis_size("ens")
    if n_batch != 2 or w1.shape[0] != 1 or n_ens & (n_ens - 1) or n_ens < 8:
        raise ValueError("unsupported mesh")
    states = per_dev * n_batch
    block = 2 * states
    half = hidden // n_batch
    nact = action_table.shape[0]
    cols = (samples + 2) * states
    samp_cols = cols - block
    inner = nact + 2 * block
    chunks = half // CHUNK
    piece = per_dev * width // LANES // n_ens
    vmem = pl.BlockSpec(memory_space=pltpu.VMEM)
    anywhere = pl.BlockSpec(memory_space=pl.ANY)
    hbm = pl.BlockSpec(memory_space=pltpu.HBM)
    dma = pltpu.SemaphoreType.DMA
    lhs, rhs, gv, stats = pl.pallas_call(
        functools.partial(kernel, n_ens, per_dev, samples, n_ens * w1.shape[0]),
        out_shape=(
            pltpu.VMEM((half, inner), BF16),
            pltpu.VMEM((nact + 6 * states, width), BF16),
            jax.ShapeDtypeStruct((1, half), F32),
            jax.ShapeDtypeStruct((1, 3), F32),
        ),
        in_specs=[vmem] * 7 + [hbm] * 4,
        out_specs=(vmem,) * 4,
        scratch_shapes=[
            pltpu.VMEM(replay_obs.shape, BF16),
            pltpu.VMEM(replay_next.shape, BF16),
            pltpu.VMEM(action_table.shape, BF16),
            pltpu.VMEM((1, cols), jnp.int32),
            pltpu.VMEM((2, block), F32),
            pltpu.VMEM((half, width), BF16),
            pltpu.VMEM((states, width), BF16),
            pltpu.VMEM((states, width), BF16),
            pltpu.VMEM((states, width), BF16),
            pltpu.VMEM((2, 2 * block, width), BF16),
            pltpu.VMEM((2, block, width), BF16),
            pltpu.VMEM((1, cols), jnp.int32),
            pltpu.VMEM((2, block), F32),
            pltpu.VMEM((nact + block, samp_cols), BF16),
            pltpu.VMEM((nact + block, samp_cols), BF16),
            pltpu.VMEM((half, nact), BF16),
            pltpu.VMEM((CHUNK, samp_cols), F32),
            pltpu.VMEM((CHUNK, samp_cols), F32),
            pltpu.VMEM((half, block), F32),
            pltpu.VMEM((half // 2, block), F32),
            pltpu.VMEM((half, LANES), F32),
            pltpu.VMEM((states, half), BF16),
            pltpu.VMEM((half, samp_cols), BF16),
            pltpu.VMEM((half, samp_cols), BF16),
            pltpu.VMEM((states, width), F32),
            pltpu.VMEM((states, width), BF16),
            pltpu.VMEM((states, width), BF16),
            pltpu.VMEM((1, cols), F32),
            pltpu.VMEM((1, cols), F32),
            pltpu.VMEM((per_dev, width), F32),
            pltpu.VMEM((n_ens, piece, LANES), BF16),
            pltpu.VMEM((n_ens, piece, LANES), BF16),
            pltpu.VMEM((8, block), F32),
            pltpu.VMEM((n_ens, 8, block), F32),
            pltpu.VMEM((piece, LANES), BF16),
            pltpu.VMEM((2, n_ens, piece, LANES), BF16),
            pltpu.VMEM((states, width), F32),
            pltpu.VMEM((half // 2, block), F32),
            pltpu.VMEM((1, half), F32),
            pltpu.VMEM((states, width), F32),
            dma((3,)), dma((chunks,)),
            dma((4,)), dma((4,)), dma((4,)), dma((4,)),
            dma((n_ens,)), dma((n_ens,)), dma((n_ens,)), dma((n_ens,)), dma((2, n_ens)), dma((2, n_ens)),
            pltpu.SemaphoreType.REGULAR((n_ens.bit_length() + 1,)),
        ],
        compiler_params=pltpu.CompilerParams(
            collective_id=0, has_side_effects=True, vmem_limit_bytes=VMEM_LIMIT
        ),
    )(*(
        pltpu.with_memory_space_constraint(x, pltpu.HBM)
        for x in (
            batch_rows[None], next_action[None], data_action[None],
            sampled_actions.T, reward[None], next_logp[None], w2,
            replay_obs, replay_next, action_table, w1,
        )
    ))
    swapped = lax.ppermute(gv, "batch", [(0, 1), (1, 0)])
    first = lax.axis_index("batch") == 0
    grad_w2 = jnp.concatenate(
        [jnp.where(first, gv, swapped), jnp.where(first, swapped, gv)], axis=1
    )
    grad_w1, stats = pl.pallas_call(
        functools.partial(finish, nact),
        out_shape=(
            jax.ShapeDtypeStruct((1, half, width), F32),
            jax.ShapeDtypeStruct((1, 3), F32),
        ),
        in_specs=[vmem] * 3,
        out_specs=(hbm, vmem),
        scratch_shapes=[pltpu.VMEM((half, width), F32), dma((4,))],
        compiler_params=pltpu.CompilerParams(vmem_limit_bytes=VMEM_LIMIT_2),
        cost_estimate=pl.CostEstimate(
            flops=2 * half * width * inner, bytes_accessed=4 * half * width, transcendentals=0
        ),
    )(lhs, rhs, stats)
    return grad_w1, grad_w2, stats


def solution(mesh):
    return jax.shard_map(
        body,
        mesh=mesh,
        in_specs=(
            P("batch", None),
            P("batch", None),
            P("batch"),
            P("batch"),
            P("batch"),
            P("batch", None),
            P("batch"),
            P("batch"),
            P(),
            P("ens", None, None),
            P("ens", None),
        ),
        out_specs=(P("ens", "batch", None), P("ens", None), P("ens", None)),
        check_vma=False,
    )
```

```python
import functools

import jax
import jax.numpy as jnp
from jax import lax
from jax.experimental import pallas as pl
from jax.experimental.pallas import tpu as pltpu
from jax.sharding import PartitionSpec as P

discount = 0.99
entropy_temp = 0.2
penalty_weight = 1.0
diversity_weight = 1000.0

MESH = pl.DeviceIdType.MESH
F32 = jnp.float32
BF16 = jnp.bfloat16
CHUNK = 256
LANES = 128
VMEM_LIMIT = 36 * 1024 * 1024
VMEM_LIMIT_2 = 24 * 1024 * 1024


def dot_t(a, b):
    return lax.dot_general(a, b, (((1,), (1,)), ((), ())), preferred_element_type=F32)


def sigmoid(x):
    return 0.5 * jnp.tanh(0.5 * x) + 0.5


open_phase = [None]
def phase(name):
    if open_phase[0] is not None:
        open_phase[0].__exit__(None,None,None)
        open_phase[0]=None
    if name:
        open_phase[0]=jax.named_scope(name); open_phase[0].__enter__()

def kernel(
    n_ens, per_dev, samples, critics_total,
    rows_ref, next_act_ref, data_act_ref, samp_act_ref, reward_ref, logp_ref, w2_ref,
    obs_hbm, next_hbm, table_hbm, w1_ref,
    lhs, rhs, gv_ref, stat_ref,
    obs_ref, next_ref, table_ref, acts_ref, aux_ref, wbuf, xobs, xnext, xdat, xin, xnx, acts_in, aux_in, sel, sel_dq, ptab,
    pbuf_a, pbuf_b, base, pcat, vb, cot, sbuf, ubuf,
    gpart, gsend, grecv, qpart, qrecv, unit, usend, urecv, qmine, qall, spread_mine, spread_all, spread,
    dcoef_buf, gvsamp, tabd,
    in_sem, w_sem, a_send, a_recv, g_send, g_recv, u_send, u_recv, m_send, m_recv, s_send, s_recv,
    known,
):
    e = lax.axis_index("ens")
    b = lax.axis_index("batch")
    peer = 1 - b
    states = 2 * per_dev
    block = 2 * states
    nact = table_ref.shape[0]
    width = table_ref.shape[1]
    half_width = width // 2
    cols = acts_ref.shape[1]
    samp_cols = cols - block
    groups = samp_cols // LANES
    half = wbuf.shape[0]
    chunks = half // CHUNK
    pairs = chunks // 2
    pair = {"ens": e, "batch": peer}

    def other(k):
        return {"ens": lax.rem(e + k, n_ens), "batch": b}

    levels = n_ens.bit_length() - 1
    cube = levels - 1
    line = n_ens // 4
    z = lax.div(e, line)
    middle = jnp.logical_and(z >= 1, z <= 2)

    def at_ens(k):
        return {"ens": k, "batch": b}

    partners = [at_ens(e + (1 << k) * (1 - 2 * (lax.div(e, 1 << k) % 2))) for k in range(cube)]
    across = at_ens(e + line * (3 - 2 * z))
    barrier = pltpu.get_barrier_semaphore()
    for to in partners + [pair]:
        pl.semaphore_signal(barrier, inc=1, device_id=to, device_id_type=MESH)

    @pl.when(middle)
    def greet_across():
        pl.semaphore_signal(barrier, inc=1, device_id=across, device_id_type=MESH)

    def tell(k, to):
        pl.semaphore_signal(known.at[k], inc=1, device_id=to, device_id_type=MESH)

    def hear(k):
        pl.semaphore_wait(known.at[k], 1)

    def advance(first_level, last_level):
        for k in range(first_level, last_level):
            hear(k)
            if k + 1 < cube:
                tell(k + 1, partners[k + 1])

    def cross_tell():
        @pl.when(middle)
        def go():
            tell(cube, across)

    def cross_hear():
        @pl.when(middle)
        def go():
            hear(cube)
            tell(cube + 1, partners[cube - 1])

    def edge_hear():
        @pl.when(jnp.logical_not(middle))
        def go():
            hear(cube + 1)

        tell(cube + 2, pair)

    third = -(-cube // 3)
    marks = [min(cube, third * k) for k in range(4)]
    loads = [
        pltpu.make_async_copy(obs_hbm, obs_ref, in_sem.at[0]),
        pltpu.make_async_copy(table_hbm, table_ref, in_sem.at[1]),
        pltpu.make_async_copy(next_hbm, next_ref, in_sem.at[2]),
    ]
    for copy in loads:
        copy.start()

    def w_copy(c):
        return pltpu.make_async_copy(
            w1_ref.at[0, pl.ds(b * half + c * CHUNK, CHUNK), :],
            wbuf.at[pl.ds(c * CHUNK, CHUNK), :],
            w_sem.at[c],
        )

    d_top = nact + 3 * states
    own_rows = pl.ds(pl.multiple_of(b * per_dev, per_dev), per_dev)
    peer_rows = pl.ds(pl.multiple_of(peer * per_dev, per_dev), per_dev)

    def one_hot(index_row, length):
        row = jnp.concatenate([index_row, jnp.zeros((1, LANES - per_dev), jnp.int32)], axis=1)
        hit = row == lax.broadcasted_iota(jnp.int32, (length, LANES), 0)
        return jnp.transpose(jnp.where(hit, 1.0, 0.0))[:per_dev, :].astype(BF16)

    phase("indices")
    pick = one_hot(rows_ref[...], obs_ref.shape[0])
    act_rows = [next_act_ref[...], data_act_ref[...]]
    act_rows += [samp_act_ref[i:i + 1, :] for i in range(samples)]

    def place(part):
        return [jnp.where(b == 0, part, jnp.zeros_like(part)), jnp.where(b == 0, jnp.zeros_like(part), part)]

    for j in range(cols // block):
        acts_ref[:, j * block:(j + 1) * block] = jnp.concatenate(
            place(act_rows[2 * j]) + place(act_rows[2 * j + 1]), axis=1
        )
    aux_ref[0:1, :] = jnp.concatenate(place(reward_ref[...]) * 2, axis=1)
    aux_ref[1:2, :] = jnp.concatenate(place(logp_ref[...]) * 2, axis=1)
    for c in range(chunks):
        w_copy(c).start()
    phase("readout")
    for g in range(pairs):
        v_row = w2_ref[0:1, pl.ds(pl.multiple_of(b * half + 2 * g * CHUNK, CHUNK), 2 * CHUNK)]
        vb[2 * g * CHUNK:2 * (g + 1) * CHUNK, :] = jnp.transpose(jnp.broadcast_to(v_row, (LANES, 2 * CHUNK)))
    for i in range(2):
        gap = slice((1 - i) * states, (2 - i) * states)
        xin[i, gap, :] = jnp.zeros((states, width), BF16)
        xnx[i, gap, :] = jnp.zeros((states, width), BF16)
        rhs[d_top + 2 * i * states:d_top + (2 * i + 1) * states, :] = jnp.zeros((states, width), BF16)
    phase("observations")
    loads[0].wait()
    xobs[own_rows, :] = jnp.dot(pick, obs_ref[...], preferred_element_type=F32).astype(BF16)
    phase("entry")
    pl.semaphore_wait(barrier, len(partners) + 1 + jnp.where(middle, 1, 0))
    tell(0, partners[0])

    def remote(src, dst, send, recv, to):
        return pltpu.make_async_remote_copy(
            src_ref=src, dst_ref=dst, send_sem=send, recv_sem=recv,
            device_id=to, device_id_type=MESH,
        )

    first = [
        remote(acts_ref, acts_in, a_send.at[0], a_recv.at[0], pair),
        remote(xobs.at[own_rows, :], xobs.at[own_rows, :], a_send.at[1], a_recv.at[1], pair),
        remote(xnext.at[own_rows, :], xnext.at[own_rows, :], a_send.at[2], a_recv.at[2], pair),
        remote(aux_ref, aux_in, a_send.at[3], a_recv.at[3], pair),
    ]
    phase("next_rows")
    first[0].start()
    first[1].start()
    loads[1].wait()
    moved = jnp.dot(one_hot(next_act_ref[...], nact), table_ref[...], preferred_element_type=F32)
    loads[2].wait()
    moved = moved + jnp.dot(pick, next_ref[...], preferred_element_type=F32)
    xnext[own_rows, :] = moved.astype(BF16)
    first[2].start()
    first[3].start()

    phase("main")
    for g in range(pairs):
        w_copy(2 * g).wait()
        w_copy(2 * g + 1).wait()
        rows = [slice((2 * g + i) * CHUNK, (2 * g + i + 1) * CHUNK) for i in range(2)]
        made = [dot_t(wbuf[r, :], table_ref[...]) for r in rows]
        for r, out in zip(rows, made):
            ptab[r, :] = (0.5 * out).astype(BF16)

    phase("greetings")
    advance(marks[0], marks[1])
    first[0].wait()
    acts = acts_ref[...] + acts_in[...]
    hit = acts[:, :block] == lax.broadcasted_iota(jnp.int32, (nact, block), 0)
    picked = jnp.transpose(jnp.where(hit, 1.0, 0.0))[states:, :].astype(BF16)
    tabd[...] = jnp.dot(picked, table_ref[...], preferred_element_type=F32)
    advance(marks[1], marks[2])
    lane = lax.broadcasted_iota(jnp.int32, (1, block), 1)
    low = lane < states
    first[1].wait()
    obs_rows = xobs[...]
    data_rows = (obs_rows.astype(F32) + tabd[...]).astype(BF16)
    xdat[...] = data_rows
    for i in range(2):
        xin[i, i * states:(i + 1) * states, :] = data_rows
        xin[i, block:block + states, :] = obs_rows
        xin[i, block + states:, :] = obs_rows

    def chunk_rows(c):
        return slice(c * CHUNK, (c + 1) * CHUNK)

    def both(k, lhs_pair):
        one = dot_t(wbuf[chunk_rows(k), :], lhs_pair[0][...])
        two = dot_t(wbuf[chunk_rows(k + pairs), :], lhs_pair[1][...])
        return one, two

    def both_v(k):
        return jnp.where(low, vb[chunk_rows(k), :], vb[chunk_rows(k + pairs), :])

    def data_matmul(k):
        one, two = both(k, (xin.at[0], xin.at[1]))
        pcat[chunk_rows(k), :] = one[:, :block] + two[:, :block]
        base[chunk_rows(k), :] = 0.5 * one[:, block:]
        base[chunk_rows(k + pairs), :] = 0.5 * two[:, block:]

    def data_forward(k, q_acc):
        pre = pcat[chunk_rows(k), :]
        v = both_v(k)
        sig = sigmoid(pre)
        silu = pre * sig
        weighted = v * (sig * (1.0 + (pre - silu)))
        flat = jnp.transpose(weighted)
        for i in range(2):
            rows = chunk_rows(k + i * pairs)
            lhs[rows, nact + block:] = weighted.astype(BF16)
            cot[:, rows] = flat[i * states:(i + 1) * states, :].astype(BF16)
        return q_acc + jnp.sum(silu * v, axis=0, keepdims=True)

    q_data = jnp.zeros((1, block), F32)
    data_matmul(0)
    for k in range(pairs):
        if k + 1 < pairs:
            data_matmul(k + 1)
        q_data = data_forward(k, q_data)
    q_data = q_data + pltpu.roll(q_data, states, 1)
    second = [
        remote(qpart.at[:, :block], qrecv.at[:, :block], g_send.at[0], g_recv.at[0], pair),
        remote(gsend.at[peer_rows, :half_width], grecv.at[peer_rows, :half_width], g_send.at[1], g_recv.at[1], pair),
        remote(qpart.at[:, block:], qrecv.at[:, block:], g_send.at[2], g_recv.at[2], pair),
        remote(gsend.at[own_rows, :], grecv.at[own_rows, :], g_send.at[3], g_recv.at[3], pair),
        remote(gsend.at[peer_rows, half_width:], grecv.at[peer_rows, half_width:], g_send.at[4], g_recv.at[4], pair),
    ]

    def grad_columns(at, copy):
        @pl.when(e >= 0)
        def go():
            made = jnp.dot(cot[...], wbuf[:, at], preferred_element_type=F32)
            gpart[:, at] = made
            gsend[:, at] = made.astype(BF16)
            copy.start()

    grad_columns(slice(0, half_width), second[1])
    grad_columns(slice(half_width, width), second[4])
    advance(marks[2], marks[3])
    cross_tell()
    row = lax.broadcasted_iota(jnp.int32, (nact + block, LANES), 0)
    own_state = lax.rem(lax.broadcasted_iota(jnp.int32, (nact + block, LANES), 1), states)
    own_state = jnp.logical_and(row >= nact, lax.rem(row - nact, states) == own_state)
    for j in range(groups):
        hit = jnp.logical_or(row == acts[:, block + j * LANES:block + (j + 1) * LANES], own_state)
        sel[:, j * LANES:(j + 1) * LANES] = jnp.where(hit, 1.0, 0.0).astype(BF16)

    rhs[:nact, :] = table_ref[...]
    rhs[nact:nact + states, :] = xdat[...]
    rhs[nact + states:nact + block, :] = xobs[...]
    rhs[nact + block:d_top, :] = xdat[...]

    first[2].wait()
    for i in range(2):
        xnx[i, i * states:(i + 1) * states, :] = xnext[...]

    def next_matmul(k):
        one, two = both(k, (xnx.at[0], xnx.at[1]))
        dcoef_buf[chunk_rows(k), :] = one + two

    q_next = jnp.zeros((1, block), F32)
    next_matmul(0)
    for k in range(pairs):
        if k + 1 < pairs:
            next_matmul(k + 1)
        pre = dcoef_buf[chunk_rows(k), :]
        q_next = q_next + jnp.sum(pre * sigmoid(pre) * both_v(k), axis=0, keepdims=True)
    q_next = q_next + pltpu.roll(q_next, states, 1)
    qpart[:, :block] = jnp.where(low, q_next, q_data)
    second[0].start()
    second[3].start()
    cross_hear()

    def samp_matmul(c, buf):
        rows = pl.ds(pl.multiple_of(c * CHUNK, CHUNK), CHUNK)
        buf[...] = jnp.dot(ptab[rows, :], sel[:nact, :], preferred_element_type=F32)

    SUB = 32

    def samp_forward(c, buf, q_acc):
        q_acc = list(q_acc)
        for r in range(CHUNK // SUB):
            here = slice(r * SUB, (r + 1) * SUB)
            there = pl.ds(pl.multiple_of(c * CHUNK + r * SUB, SUB), SUB)
            v = vb[there, :]
            start = base[there, :]
            for j in range(groups):
                at = slice(j * LANES, (j + 1) * LANES)
                h = buf[here, at] + start
                t = jnp.tanh(h)
                m = h * t
                silu = h + m
                slope = (1.0 + t) * (1.0 + (h - m))
                sbuf[there, at] = slope.astype(BF16)
                ubuf[there, at] = silu.astype(BF16)
                sv = silu * v
                part = sv[0:8]
                for i in range(1, SUB // 8):
                    part = part + sv[8 * i:8 * i + 8]
                q_acc[j] = q_acc[j] + part
        return tuple(q_acc)

    def samp_pair(k, q_acc):
        samp_matmul(2 * k + 1, pbuf_b)
        q_acc = samp_forward(2 * k, pbuf_a, q_acc)
        samp_matmul(lax.rem(2 * k + 2, chunks), pbuf_a)
        return samp_forward(2 * k + 1, pbuf_b, q_acc)

    q_acc = (jnp.zeros((8, LANES), F32),) * groups
    cut_one = chunks // 8

    def q_copy(k):
        return remote(qmine, qall.at[k], m_send.at[k], m_recv.at[k], other(k))

    def u_copy(k):
        return remote(
            usend.at[lax.rem(e + k, n_ens)], urecv.at[k], u_send.at[k], u_recv.at[k], other(k)
        )

    def s_copy(k):
        return remote(spread_mine, spread_all.at[b, e], s_send.at[0, k], s_recv.at[0, k], other(k))

    def s_cross(k):
        to = {"ens": lax.rem(e + k, n_ens), "batch": peer}
        return remote(spread_mine, spread_all.at[b, e], s_send.at[1, k], s_recv.at[1, k], to)

    def start_all(make, begin=1):
        def go(k, carry):
            make(k).start()
            return carry
        lax.fori_loop(begin, n_ens, go, 0)

    def wait_all(make, begin=1):
        def go(k, carry):
            make(k).wait()
            return carry
        lax.fori_loop(begin, n_ens, go, 0)

    second[1].wait()
    second[4].wait()
    grad_in = gpart[own_rows, :] + grecv[own_rows, :].astype(F32)
    edge_hear()
    unit[...] = grad_in / jnp.sqrt(jnp.sum(grad_in * grad_in, axis=-1, keepdims=True) + 1.0)
    piece = usend.shape[1]
    per_col = per_dev // piece
    for p in range(n_ens):
        c0, r0 = p // per_col, (p % per_col) * piece
        usend[p] = unit[r0:r0 + piece, c0 * LANES:(c0 + 1) * LANES].astype(BF16)
    start_all(u_copy)
    samp_matmul(0, pbuf_a)
    q_acc = lax.fori_loop(0, cut_one, samp_pair, q_acc)
    second[0].wait()
    q0 = qpart[:, :block] + qrecv[:, :block]
    qmine[...] = jnp.broadcast_to(q0, qmine.shape)
    start_all(q_copy)

    q_acc = lax.fori_loop(cut_one, chunks // 2, samp_pair, q_acc)
    for j in range(groups):
        qpart[:, block + j * LANES:block + (j + 1) * LANES] = jnp.sum(q_acc[j], axis=0, keepdims=True)
    second[2].start()

    hear(cube + 2)
    wait_all(u_copy)
    total = usend[e].astype(F32)
    for k in range(1, n_ens):
        total = total + urecv[k].astype(F32)
    spread_mine[...] = total.astype(BF16)
    spread_all[b, e] = total.astype(BF16)
    start_all(s_cross, 0)
    start_all(s_copy)
    second[2].wait()
    q_samp = qpart[:, block:] + qrecv[:, block:]
    exps = jnp.exp(q_samp)
    mass = exps[:, :block]
    for j in range(1, groups):
        mass = mass + exps[:, j * block:(j + 1) * block]
    mass = mass + pltpu.roll(mass, states, 1)
    log_mass = jnp.log(mass)
    tiled = jnp.concatenate([log_mass] * groups, axis=1)
    dq_samp = penalty_weight * jnp.exp(q_samp - tiled) / states
    for j in range(groups):
        at = slice(j * LANES, (j + 1) * LANES)
        sel_dq[:, at] = (sel[:, at].astype(F32) * (0.5 * dq_samp[:, at])).astype(BF16)

    def samp_gv(c):
        there = slice(c * LANES, (c + 1) * LANES)
        total = ubuf[there, :LANES].astype(F32) * dq_samp[:, :LANES]
        for j in range(1, groups):
            at = slice(j * LANES, (j + 1) * LANES)
            total = total + ubuf[there, at].astype(F32) * dq_samp[:, at]
        gvsamp[:, there] = jnp.sum(jnp.transpose(total), axis=0, keepdims=True)

    mid = slice(nact, nact + block)

    def samp_step(k):
        rows = slice(k * 2 * CHUNK, (k + 1) * 2 * CHUNK)
        grads = dot_t(sbuf[rows, :], sel_dq[...])
        v = vb[rows, :]
        for j in range(nact // LANES):
            at = slice(j * LANES, (j + 1) * LANES)
            lhs[rows, at] = (v * grads[:, at]).astype(BF16)
        lhs[rows, mid] = (v * grads[:, mid]).astype(BF16)

    steps = chunks // 2
    share = half // LANES // steps
    for k in range(steps):
        samp_step(k)
        for c in range(k * share, (k + 1) * share):
            samp_gv(c)
    wait_all(q_copy)
    floor = qmine[...]
    for k in range(1, n_ens):
        floor = jnp.minimum(floor, qall[k])
    floor = floor[0:1, :]
    floor = jnp.where(low, floor, pltpu.roll(floor, states, 1))
    q_own = jnp.where(low, pltpu.roll(q0, states, 1), q0)
    first[3].wait()
    aux = aux_ref[...] + aux_in[...]
    target = aux[0:1, :] + discount * (floor - entropy_temp * aux[1:2, :])
    td_gap = q_own - target
    dq_data = (2.0 * td_gap - penalty_weight) / states

    second[3].wait()
    grad_in = gpart[...] + grecv[...].astype(F32)
    in_norm = jnp.sqrt(jnp.sum(grad_in * grad_in, axis=-1, keepdims=True) + 1.0)
    unit_dir = grad_in / in_norm
    wait_all(s_cross, 0)
    wait_all(s_copy)
    scale = 2.0 * diversity_weight / (critics_total - 1) / states
    for i in range(2):
        for p in range(n_ens):
            c0, r0 = p // per_col, i * per_dev + (p % per_col) * piece
            spread[r0:r0 + piece, c0 * LANES:(c0 + 1) * LANES] = spread_all[i, p].astype(F32)
    away = spread[...] - unit_dir
    div_row = jnp.sum(unit_dir * away, axis=-1, keepdims=True)
    dgrad_rows = (scale * (away - unit_dir * div_row) / in_norm).astype(BF16)
    rhs[d_top + states:d_top + 2 * states, :] = dgrad_rows
    shifted = (rhs.at[d_top + states:, :], rhs.at[d_top:d_top + block, :])

    def dcoef_matmul(k):
        one, two = both(k, shifted)
        dcoef_buf[chunk_rows(k), :] = one + two

    def data_backward(k):
        dcoef = dcoef_buf[chunk_rows(k), :]
        pre = pcat[chunk_rows(k), :]
        v = both_v(k)
        sig = sigmoid(pre)
        silu = pre * sig
        slope = sig * (1.0 + (pre - silu))
        curve = sig * (1.0 - sig) * (2.0 + pre * (1.0 - 2.0 * sig))
        dpre = v * (dq_data * slope + dcoef * curve)
        rows = chunk_rows(k)
        lhs[rows, mid] = jnp.where(low, dpre, lhs[rows, mid].astype(F32)).astype(BF16)
        rows = chunk_rows(k + pairs)
        lhs[rows, mid] = jnp.where(low, lhs[rows, mid].astype(F32), dpre).astype(BF16)
        flat = jnp.transpose(dq_data * silu + dcoef * slope)
        for i in range(2):
            c = k + i * pairs
            late = jnp.sum(flat[i * states:(i + 1) * states, :], axis=0, keepdims=True)
            gv_ref[:, chunk_rows(c)] = gvsamp[:, chunk_rows(c)] + late

    dcoef_matmul(0)
    for k in range(pairs):
        if k + 1 < pairs:
            dcoef_matmul(k + 1)
        data_backward(k)
    td_total = jnp.sum(jnp.where(low, td_gap * td_gap, 0.0), axis=1, keepdims=True)
    gap_total = jnp.sum(jnp.where(low, log_mass - q_own, 0.0), axis=1, keepdims=True)
    div_total = jnp.sum(div_row, axis=0, keepdims=True)
    stats = jnp.where(lane == 0, td_total, jnp.where(lane == 1, gap_total, div_total))
    stat_ref[...] = (stats / states)[:, :3]
    phase(None)


def finish(nact, lhs_ref, rhs_ref, stat_ref, out_hbm, stat_out, buf, sem):
    stat_out[...] = stat_ref[...]
    parts = sem.shape[0]
    tile = buf.shape[0] // parts
    states = (lhs_ref.shape[1] - nact) // 4
    block = 2 * states
    mids = []
    for i in range(2):
        x_top = nact + i * states
        d_top = nact + block + (2 - i) * states
        mids.append(jnp.concatenate([rhs_ref[x_top:x_top + block, :], rhs_ref[d_top:d_top + block, :]], axis=0))
    copies = []
    for i in range(parts):
        rows = pl.ds(i * tile, tile)
        out = jnp.dot(lhs_ref[rows, :nact], rhs_ref[:nact, :], preferred_element_type=F32)
        out += jnp.dot(lhs_ref[rows, nact:], mids[2 * i // parts], preferred_element_type=F32)
        buf[rows, :] = out
        copies.append(pltpu.make_async_copy(buf.at[rows, :], out_hbm.at[0, rows, :], sem.at[i]))
        copies[-1].start()
    for copy in copies:
        copy.wait()


def body(
    replay_obs, replay_next, batch_rows, data_action, next_action, sampled_actions,
    reward, next_logp, action_table, w1, w2,
):
    per_dev = batch_rows.shape[0]
    samples = sampled_actions.shape[1]
    width = replay_obs.shape[1]
    hidden = w1.shape[1]
    n_batch = lax.axis_size("batch")
    n_ens = lax.axis_size("ens")
    if n_batch != 2 or w1.shape[0] != 1 or n_ens & (n_ens - 1) or n_ens < 8:
        raise ValueError("unsupported mesh")
    states = per_dev * n_batch
    block = 2 * states
    half = hidden // n_batch
    nact = action_table.shape[0]
    cols = (samples + 2) * states
    samp_cols = cols - block
    inner = nact + 2 * block
    chunks = half // CHUNK
    piece = per_dev * width // LANES // n_ens
    vmem = pl.BlockSpec(memory_space=pltpu.VMEM)
    anywhere = pl.BlockSpec(memory_space=pl.ANY)
    hbm = pl.BlockSpec(memory_space=pltpu.HBM)
    dma = pltpu.SemaphoreType.DMA
    lhs, rhs, gv, stats = pl.pallas_call(
        functools.partial(kernel, n_ens, per_dev, samples, n_ens * w1.shape[0]),
        out_shape=(
            pltpu.VMEM((half, inner), BF16),
            pltpu.VMEM((nact + 6 * states, width), BF16),
            jax.ShapeDtypeStruct((1, half), F32),
            jax.ShapeDtypeStruct((1, 3), F32),
        ),
        in_specs=[vmem] * 7 + [hbm] * 4,
        out_specs=(vmem,) * 4,
        scratch_shapes=[
            pltpu.VMEM(replay_obs.shape, BF16),
            pltpu.VMEM(replay_next.shape, BF16),
            pltpu.VMEM(action_table.shape, BF16),
            pltpu.VMEM((1, cols), jnp.int32),
            pltpu.VMEM((2, block), F32),
            pltpu.VMEM((half, width), BF16),
            pltpu.VMEM((states, width), BF16),
            pltpu.VMEM((states, width), BF16),
            pltpu.VMEM((states, width), BF16),
            pltpu.VMEM((2, 2 * block, width), BF16),
            pltpu.VMEM((2, block, width), BF16),
            pltpu.VMEM((1, cols), jnp.int32),
            pltpu.VMEM((2, block), F32),
            pltpu.VMEM((nact + block, samp_cols), BF16),
            pltpu.VMEM((nact + block, samp_cols), BF16),
            pltpu.VMEM((half, nact), BF16),
            pltpu.VMEM((CHUNK, samp_cols), F32),
            pltpu.VMEM((CHUNK, samp_cols), F32),
            pltpu.VMEM((half, block), F32),
            pltpu.VMEM((half // 2, block), F32),
            pltpu.VMEM((half, LANES), F32),
            pltpu.VMEM((states, half), BF16),
            pltpu.VMEM((half, samp_cols), BF16),
            pltpu.VMEM((half, samp_cols), BF16),
            pltpu.VMEM((states, width), F32),
            pltpu.VMEM((states, width), BF16),
            pltpu.VMEM((states, width), BF16),
            pltpu.VMEM((1, cols), F32),
            pltpu.VMEM((1, cols), F32),
            pltpu.VMEM((per_dev, width), F32),
            pltpu.VMEM((n_ens, piece, LANES), BF16),
            pltpu.VMEM((n_ens, piece, LANES), BF16),
            pltpu.VMEM((8, block), F32),
            pltpu.VMEM((n_ens, 8, block), F32),
            pltpu.VMEM((piece, LANES), BF16),
            pltpu.VMEM((2, n_ens, piece, LANES), BF16),
            pltpu.VMEM((states, width), F32),
            pltpu.VMEM((half // 2, block), F32),
            pltpu.VMEM((1, half), F32),
            pltpu.VMEM((states, width), F32),
            dma((3,)), dma((chunks,)),
            dma((4,)), dma((4,)), dma((5,)), dma((5,)),
            dma((n_ens,)), dma((n_ens,)), dma((n_ens,)), dma((n_ens,)), dma((2, n_ens)), dma((2, n_ens)),
            pltpu.SemaphoreType.REGULAR((n_ens.bit_length() + 1,)),
        ],
        compiler_params=pltpu.CompilerParams(
            collective_id=0, has_side_effects=True, vmem_limit_bytes=VMEM_LIMIT
        ),
    )(*(
        pltpu.with_memory_space_constraint(x, pltpu.HBM)
        for x in (
            batch_rows[None], next_action[None], data_action[None],
            sampled_actions.T, reward[None], next_logp[None], w2,
            replay_obs, replay_next, action_table, w1,
        )
    ))
    swapped = lax.ppermute(gv, "batch", [(0, 1), (1, 0)])
    first = lax.axis_index("batch") == 0
    grad_w2 = jnp.concatenate(
        [jnp.where(first, gv, swapped), jnp.where(first, swapped, gv)], axis=1
    )
    grad_w1, stats = pl.pallas_call(
        functools.partial(finish, nact),
        out_shape=(
            jax.ShapeDtypeStruct((1, half, width), F32),
            jax.ShapeDtypeStruct((1, 3), F32),
        ),
        in_specs=[vmem] * 3,
        out_specs=(hbm, vmem),
        scratch_shapes=[pltpu.VMEM((half, width), F32), dma((4,))],
        compiler_params=pltpu.CompilerParams(vmem_limit_bytes=VMEM_LIMIT_2),
        cost_estimate=pl.CostEstimate(
            flops=2 * half * width * inner, bytes_accessed=4 * half * width, transcendentals=0
        ),
    )(lhs, rhs, stats)
    return grad_w1, grad_w2, stats


def solution(mesh):
    return jax.shard_map(
        body,
        mesh=mesh,
        in_specs=(
            P("batch", None),
            P("batch", None),
            P("batch"),
            P("batch"),
            P("batch"),
            P("batch", None),
            P("batch"),
            P("batch"),
            P(),
            P("ens", None, None),
            P("ens", None),
        ),
        out_specs=(P("ens", "batch", None), P("ens", None), P("ens", None)),
        check_vma=False,
    )
```
